32 devices in a mesh: dom: 32 (over z, y, x, core).
Axes of the slice: x: 2, y: 2, z: 4, core: 2. Of those that a mesh axis runs over, the one named last changes fastest.
Arguments:
- particles: bfloat16 [1024, 2, 7488], P('dom'), may hold values from -6 to 6
- references: bfloat16 [32, 2, 7488], P('dom'), may hold values from -6 to 6
- assignment: int32 [1024, 1], P('dom'), may hold values from 0 to 31
- orientation: int32 [1024], P('dom'), may hold values from 0 to 35
- tilt_range: int32 [2, 1024], P(None, 'dom'), may hold values from 0 to 20
Outputs:
- scores: float32 [1024, 32], P('dom')
- class_means: float32 [32, 2, 7488], P('dom')
- class_load: float32 [32], replicated
The draws below stay inside these ranges and needn't reach their ends.
Inputs may be any that keep to these rules, and one draw needn't show every extreme that they name: `assignment`: every class has at least one particle.
All inputs are finite; a program needn't handle non-finite values.
Results may differ from the reference program's by a relative error of at most 0.0035.
Values may be sent and summed in bfloat16 or wider, within the bound.
A program may use at most 128 MiB of HBM per device.

```python
import math
import jax
import jax.numpy as jnp
from jax import lax

GRID = 24
ORIENTS = 36
TILT_BINS = 21
PART_DEV = 32
CLASSES = 32
COEF = 7488
PARTICLES = 1024
N_DOM = 32


def with_ends(drawn, own_key, least, largest):
    place = [jax.random.randint(jax.random.fold_in(own_key, axis), (), 0, length) for axis, length in enumerate(drawn.shape)]
    widest = drawn.shape.index(max(drawn.shape))
    neighbour = place[:widest] + [(place[widest] + 1) % drawn.shape[widest]] + place[widest + 1:]
    return drawn.at[tuple(place)].set(least).at[tuple(neighbour)].set(largest)


def level_of(key, dims, cuts, low, largest):
    loudness = 1.0
    for axis_at, parts in cuts:
        draws = jax.random.uniform(jax.random.fold_in(jax.random.fold_in(key, 6), axis_at), (parts,), jnp.float32, low / len(cuts), largest / len(cuts))
        loudness = loudness * jnp.repeat(jnp.exp(draws), dims[axis_at] // parts).reshape((-1,) + (1,) * (len(dims) - 1 - axis_at))
    return loudness


def picks_of(rng, rows, number_of, top, lift):
    sequence = jax.random.permutation(jax.random.fold_in(rng, 1), number_of)
    boost = sequence
    for power in range(3):
        boost = boost * boost // number_of
    boost = boost * lift // number_of
    chance = jax.random.randint(jax.random.fold_in(rng, 2), (rows, number_of), 0, 4096) + boost
    holders = jax.random.permutation(jax.random.fold_in(rng, 3), rows)[jnp.arange(number_of) % rows]
    chance = jnp.where(jnp.arange(rows)[:, None] == holders[None, :], 1 << 14, chance)
    priority = chance * number_of + jnp.arange(number_of)
    return lax.top_k(priority.astype(jnp.int32), top)[1].astype(jnp.int32)


def noise(rng, shape, spread, most, pieces=(), kind=jnp.bfloat16):
    array = jax.random.normal(rng, shape, jnp.float32) * spread
    if len(pieces) > 0:
        array = level_of(rng, shape, pieces, -0.22, 0.18) * array
    return jnp.clip(array, min=-most, max=most).astype(kind)


def setup_inputs(seed: int = 0) -> dict:
    keys = jax.random.split(jax.random.key(seed), 6)
    return {
        "particles": noise(keys[0], (PARTICLES, 2, COEF), 1.0, 6.0, ((0, 32),)),
        "references": noise(keys[1], (CLASSES, 2, COEF), 1.0, 6.0, ((0, 32),)),
        "assignment": picks_of(keys[2], PARTICLES, CLASSES, 1, 256),
        "orientation": with_ends(jax.random.randint(keys[3], (PARTICLES,), 0, ORIENTS), jax.random.fold_in(keys[3], 1), 0, ORIENTS - 1).astype(jnp.int32),
        "tilt_range": with_ends(jax.random.randint(keys[4], (2, PARTICLES), 0, TILT_BINS), jax.random.fold_in(keys[4], 1), 0, TILT_BINS - 1).astype(jnp.int32),
    }


EPS = 1e-06
GAIN = 6.0
TAU = 0.5

def tables():
    index = jnp.arange(COEF, dtype=jnp.int32)
    plane = index // (GRID * GRID)
    rest = index % (GRID * GRID)
    col_x = rest // GRID
    col_z = rest % GRID
    freq_x = ((col_x + GRID // 2) % GRID - GRID // 2).astype(jnp.float32)
    freq_y = plane.astype(jnp.float32)
    freq_z = ((col_z + GRID // 2) % GRID - GRID // 2).astype(jnp.float32)
    return (freq_x, freq_y, freq_z)

def wedge_weights(orient, low_bin, high_bin):
    freq_x, freq_y, freq_z = tables()
    angle = orient.astype(jnp.float32) * (2.0 * math.pi / ORIENTS)
    along = -freq_x[None, :] * jnp.sin(angle)[:, None] + freq_y[None, :] * jnp.cos(angle)[:, None]
    radius = along * along + freq_z[None, :] * freq_z[None, :] + 1.0
    cos_two = (along * along - freq_z[None, :] * freq_z[None, :]) / radius
    sin_two = -2.0 * along * freq_z[None, :] / radius
    low = -(40.0 + 1.5 * low_bin.astype(jnp.float32)) * (math.pi / 180.0)
    high = (40.0 + 1.5 * high_bin.astype(jnp.float32)) * (math.pi / 180.0)
    centre = (low + high)[:, None]
    width = (high - low)[:, None]
    return jax.nn.sigmoid(GAIN * (cos_two * jnp.cos(centre) + sin_two * jnp.sin(centre) - jnp.cos(width)))

def reference(particles, references, assignment, orientation, tilt_range):
    ref32 = references.astype(jnp.float32)
    ref_power = (ref32[:, 0] * ref32[:, 0] + ref32[:, 1] * ref32[:, 1]).astype(jnp.bfloat16)
    ref_flat = references.reshape(CLASSES, 2 * COEF)
    part_blocks = particles.reshape(N_DOM, PART_DEV, 2, COEF)
    cls_blocks = assignment.reshape(N_DOM, PART_DEV)
    ori_blocks = orientation.reshape(N_DOM, PART_DEV)
    tilt_blocks = tilt_range.reshape(2, N_DOM, PART_DEV).transpose(1, 0, 2)
    class_ids = jnp.arange(CLASSES, dtype=jnp.int32)

    def step(carry, item):
        numer, denom, counts, totals = carry
        part, cls, ori, tilt = item
        wedge = wedge_weights(ori, tilt[0], tilt[1])
        pf = part.astype(jnp.float32)
        weighted = (wedge[:, None, :] * pf).astype(jnp.bfloat16)
        flat = weighted.reshape(PART_DEV, 2 * COEF)
        wedge_sq = (wedge * wedge).astype(jnp.bfloat16)
        wedge_low = wedge.astype(jnp.bfloat16)
        power = lax.optimization_barrier(jnp.sum(wedge * (pf[:, 0] * pf[:, 0] + pf[:, 1] * pf[:, 1]), axis=1))
        intersection = jnp.dot(flat, ref_flat.T, preferred_element_type=jnp.float32)
        energy = jnp.dot(wedge_low, ref_power.T, preferred_element_type=jnp.float32)
        scores = intersection / (math.sqrt(COEF) * jnp.sqrt((energy / COEF + EPS) * (power[:, None] / COEF + EPS)))
        onehot = (class_ids[:, None] == cls[None, :]).astype(jnp.bfloat16)
        numer = numer + jnp.dot(onehot, flat, preferred_element_type=jnp.float32)
        denom = denom + jnp.dot(onehot, wedge_sq, preferred_element_type=jnp.float32)
        onehot32 = onehot.astype(jnp.float32)
        counts = counts + lax.optimization_barrier(jnp.sum(onehot32, axis=1))
        totals = totals + jnp.dot(onehot32, lax.optimization_barrier(jnp.sum(wedge, axis=1)), precision=lax.Precision.HIGHEST)
        return ((numer, denom, counts, totals), scores)
    start = (jnp.zeros((CLASSES, 2 * COEF), jnp.float32), jnp.zeros((CLASSES, COEF), jnp.float32), jnp.zeros((CLASSES,), jnp.float32), jnp.zeros((CLASSES,), jnp.float32))
    (numer, denom, counts, totals), scores = lax.scan(step, start, (part_blocks, cls_blocks, ori_blocks, tilt_blocks))
    scores = scores.reshape(PARTICLES, CLASSES)
    bottom = denom + TAU * (totals[:, None] / COEF + 1.0)
    class_means = numer.reshape(CLASSES, 2, COEF) / bottom[:, None, :]
    class_load = counts * CLASSES / PARTICLES
    return (scores, class_means, class_load)
```

```python
import functools
import math

import jax
import jax.numpy as jnp
from jax import lax
from jax.experimental import pallas as pl
from jax.experimental.pallas import tpu as pltpu
from jax.sharding import PartitionSpec as P

GRID = 24
ORIENTS = 36
EPS = 1e-06
GAIN = 6.0
TAU = 0.5
LANES = 128
MESH = pl.DeviceIdType.MESH

PAIRS = 3
CHUNKS = 2 * PAIRS
SUB = 640


def factor(devices):
    chips = devices // 2
    log = chips.bit_length() - 1
    gx = 1 << (log // 3)
    gy = 1 << ((log - log // 3) // 2)
    return gx, gy, chips // (gx * gy)


def column(row):
    rows = row.shape[1]
    line = lax.broadcasted_iota(jnp.int32, (rows, rows), 0)
    lane = lax.broadcasted_iota(jnp.int32, (rows, rows), 1)
    return jnp.sum(jnp.where(line == lane, row, 0.0), axis=1, keepdims=True)


def frequencies(first, width):
    index = (lax.broadcasted_iota(jnp.int32, (1, width), 1) + first).astype(jnp.float32)
    plane = jnp.floor((index + 0.5) * (1.0 / (GRID * GRID)))
    rest = index - plane * (GRID * GRID)
    col_x = jnp.floor((rest + 0.5) * (1.0 / GRID))
    col_z = rest - col_x * GRID
    freq_x = jnp.where(col_x >= GRID // 2, col_x - GRID, col_x)
    freq_z = jnp.where(col_z >= GRID // 2, col_z - GRID, col_z)
    return freq_x, plane, freq_z, index


def kernel(
    gx, gy, gz, span, coef, total,
    part_hbm, ref_hbm, cls_hbm, orient_hbm, tilt_hbm,
    scores_ref, means_ref, load_ref,
    part, cls_ref, orient_ref, tilt_ref,
    data, low, all_ref, mine, send_core, recv_core,
    s1x, r1x, s1y, r1y, s2x, r2x, s2y, r2y, s3, r3, small_send, small_recv,
    in_sems, ag_sems, ag_send_sem, core_sems, sems1, sems2, sems3, small_sems, send_sems,
):
    me = lax.axis_index("dom")
    core = lax.rem(me, 2)
    chip = me // 2
    x = lax.rem(chip, gx)
    y = lax.rem(chip // gx, gy)
    z = chip // (gx * gy)
    sibling = me + 1 - 2 * core
    classes = 2 * gx * gy * gz
    half = classes // 2
    rows = part.shape[0]
    wide = 3 * span
    cut = coef // 2 // LANES * LANES

    def device(x_at, y_at, z_at, c_at):
        return ((z_at * gy + y_at) * gx + x_at) * 2 + c_at

    def x_peer(j):
        return device(lax.rem(x + j, gx), y, z, core)

    def y_peer(j):
        return device(x, lax.rem(y + j, gy), z, core)

    def z_peer(j):
        return device(x, y, lax.rem(z + j, gz), core)

    def fetch(src, dst, at):
        copy = pltpu.make_async_copy(src, dst, in_sems.at[at])
        copy.start()
        return copy

    barrier = pltpu.get_barrier_semaphore()
    peers = [sibling]
    peers += [x_peer(j) for j in range(1, gx)]
    peers += [y_peer(j) for j in range(1, gy)]
    peers += [z_peer(j) for j in range(1, gz)]
    for peer in peers:
        pl.semaphore_signal(barrier, inc=1, device_id=(peer,), device_id_type=MESH)
    own_ref = fetch(ref_hbm.at[0], all_ref.at[0], 0)
    metas = [
        fetch(orient_hbm, orient_ref, 1),
        fetch(tilt_hbm, tilt_ref, 2),
        fetch(cls_hbm, cls_ref, 3),
    ]
    part_copies = []
    for p in range(PAIRS):
        first = 2 * p * span
        cols = pl.ds(first, min(2 * span, coef - first))
        part_copies.append(fetch(part_hbm.at[:, :, cols], part.at[:, :, cols], 4 + p))

    def push(src, dst, send_sem, recv_sem, target):
        pltpu.make_async_remote_copy(
            src_ref=src, dst_ref=dst, send_sem=send_sem, recv_sem=recv_sem,
            device_id=(target,), device_id_type=MESH,
        ).start()

    def whole_of(ref, sem):
        return pltpu.make_async_remote_copy(
            src_ref=ref, dst_ref=ref, send_sem=sem, recv_sem=sem,
            device_id=(sibling,), device_id_type=MESH,
        )

    def arrived(ref, sem):
        whole_of(ref, sem).wait_recv()

    def slot(dx, dy, dc):
        return ((dc * gx + dx) * gy + dy) * gz

    def give(src_slot, dst_slot, n, lanes, at, target):
        src = all_ref.at[pl.ds(src_slot, n), :, lanes]
        dst = all_ref.at[pl.ds(dst_slot, n), :, lanes]
        push(src, dst, ag_send_sem, ag_sems.at[at], target)

    every = slice(0, coef)
    front, back = slice(0, cut), slice(cut, coef)

    def ag_direct(at, n, sem):
        for j in range(1, gx):
            give(at, slot(gx - j, 0, 0) + at, n, every, sem, x_peer(j))
        for j in range(1, gy):
            give(at, slot(0, gy - j, 0) + at, n, every, sem + 1, y_peer(j))
        give(at, slot(0, 0, 1) + at, n, every, 0, sibling)

    def ag_forward(at, n, sem):
        if gx > 1:
            arrived(all_ref.at[pl.ds(0, (gx - 1) * n)], ag_sems.at[sem])
        for dx in range(1, gx):
            for j in range(1, gy):
                give(slot(dx, 0, 0) + at, slot(dx, gy - j, 0) + at, n, front, sem + 2, y_peer(j))
        if gy > 1:
            arrived(all_ref.at[pl.ds(0, (gy - 1) * n)], ag_sems.at[sem + 1])
        for dy in range(1, gy):
            for j in range(1, gx):
                give(slot(0, dy, 0) + at, slot(gx - j, dy, 0) + at, n, back, sem + 3, x_peer(j))
        for dx in range(1, gx):
            give(slot(dx, 0, 0) + at, slot(dx, 0, 1) + at, n, every, 0, sibling)
        for dy in range(1, gy):
            give(slot(0, dy, 0) + at, slot(0, dy, 1) + at, n, every, 0, sibling)

    def ag_core(at, n, sem):
        count = (gx - 1) * (gy - 1) * n
        if count:
            arrived(all_ref.at[pl.ds(0, count), :, front], ag_sems.at[sem + 2])
            arrived(all_ref.at[pl.ds(0, count), :, back], ag_sems.at[sem + 3])
        for dx in range(1, gx):
            for dy in range(1, gy):
                give(slot(dx, dy, 0) + at, slot(dx, dy, 1) + at, n, every, 0, sibling)

    def ag_own():
        own_ref.wait()
        for j in range(1, gz):
            give(0, gz - j, 1, every, 1, z_peer(j))
        ag_direct(0, 1, 2)

    def ag_rest():
        arrived(all_ref.at[pl.ds(1, gz - 1)], ag_sems.at[1])
        ag_direct(1, gz - 1, 6)

    for copy in metas:
        copy.wait()
    angle = orient_ref[...].astype(jnp.float32) * (2.0 * math.pi / ORIENTS)
    bins = tilt_ref[...].astype(jnp.float32)
    low_end = -(40.0 + 1.5 * bins[0:1]) * (math.pi / 180.0)
    high_end = (40.0 + 1.5 * bins[1:2]) * (math.pi / 180.0)
    sin_a, cos_a = column(jnp.sin(angle)), column(jnp.cos(angle))
    cos_c = column(jnp.cos(low_end + high_end))
    sin_c = column(jnp.sin(low_end + high_end))
    cos_w = column(jnp.cos(high_end - low_end))
    cls_row = cls_ref[...].astype(jnp.float32)
    cls_col = column(cls_row)

    def log2(n):
        return n.bit_length() - 1

    row = lax.broadcasted_iota(jnp.int32, (classes, 1), 0)
    row_z = row & (gz - 1)
    up = lax.shift_right_logical(row, log2(gz))
    row_c = lax.shift_right_logical(row, log2(half))

    def ids_of(dx, dy):
        return device((dx + x) & (gx - 1), (dy + y) & (gy - 1), (row_z + z) & (gz - 1), (row_c + core) & 1)

    ids = (
        ids_of(lax.shift_right_logical(up, log2(gy)) & (gx - 1), up & (gy - 1)),
        ids_of(up & (gx - 1), lax.shift_right_logical(up, log2(gx)) & (gy - 1)),
    )
    onehot = [jnp.where(i.astype(jnp.float32) == cls_row, 1.0, 0.0).astype(jnp.bfloat16) for i in ids]

    sizes = ((gx, gy), (gy, gx))
    hops = ((x_peer, y_peer), (y_peer, x_peer))
    one = ((s1x, r1x), (s1y, r1y))
    two = ((s2x, r2x), (s2y, r2y))
    sums = {"wedge": jnp.zeros((rows, 1), jnp.float32), "power": jnp.zeros((rows, 1), jnp.float32)}
    own = []

    def parts(first):
        width = max(0, min(SUB, coef - first))
        pieces = []
        if width:
            both = part[:, :, first:first + width].astype(jnp.float32)
            pieces.append(jnp.swapaxes(both, 0, 1))
        if width < SUB:
            pieces.append(jnp.zeros((2, rows, SUB - width), jnp.float32))
        both = jnp.concatenate(pieces, axis=2) if len(pieces) > 1 else pieces[0]
        return both[0], both[1]

    def compute(t):
        o = t % 2
        if o == 0:
            part_copies[t // 2].wait()
        for s in range(span // SUB):
            first = t * span + s * SUB
            freq_x, freq_y, freq_z, index = frequencies(first, SUB)
            along = freq_y * cos_a - freq_x * sin_a
            along_sq = along * along
            z_sq = freq_z * freq_z
            scale = 1.0 / (along_sq + (z_sq + 1.0))
            value = ((along_sq - z_sq) * cos_c - (2.0 * along * freq_z) * sin_c) * scale - cos_w
            wedge = 1.0 / (1.0 + jnp.exp(value * (-GAIN)))
            real, imag = parts(first)
            sums["power"] = sums["power"] + jnp.sum(wedge * (real * real + imag * imag), axis=1, keepdims=True)
            inside = wedge if first + SUB <= coef else jnp.where(index < coef, wedge, 0.0)
            sums["wedge"] = sums["wedge"] + jnp.sum(inside, axis=1, keepdims=True)
            at = s * SUB
            data[t, :, at:at + SUB] = (wedge * real).astype(jnp.bfloat16)
            data[t, :, span + at:span + at + SUB] = (wedge * imag).astype(jnp.bfloat16)
            data[t, :, 2 * span + at:2 * span + at + SUB] = (wedge * wedge).astype(jnp.bfloat16)
            low[:, first:first + SUB] = wedge.astype(jnp.bfloat16)
        for q in range(3):
            cols = slice(q * span, (q + 1) * span)
            both = jnp.dot(onehot[o], data[t, :, cols], preferred_element_type=jnp.float32)
            send_core[t, :, cols] = both[half:].astype(jnp.bfloat16)
            mine[t, :, cols] = both[:half]

    def cores(t):
        push(send_core.at[t], recv_core.at[t], send_sems.at[0], core_sems.at[t], sibling)

    def first(t):
        o, p = t % 2, t // 2
        send, recv = one[o]
        lines = sizes[o][1] * gz
        arrived(recv_core.at[t], core_sems.at[t])
        for j in range(1, sizes[o][0]):
            at = slice(j * lines, (j + 1) * lines)
            send[p, j - 1] = (mine[t, at] + recv_core[t, at].astype(jnp.float32)).astype(jnp.bfloat16)
            push(send.at[p, j - 1], recv.at[p, j - 1], send_sems.at[1 + o], sems1.at[t], hops[o][0](j))
        mine[t, :lines] = mine[t, :lines] + recv_core[t, :lines].astype(jnp.float32)

    def second(t):
        o, p = t % 2, t // 2
        lines = sizes[o][1] * gz
        recv = one[o][1]
        if sizes[o][0] > 1:
            arrived(recv.at[p], sems1.at[t])
        piece = mine[t, :lines]
        for j in range(1, sizes[o][0]):
            piece = piece + recv[p, j - 1].astype(jnp.float32)
        send, recv = two[o]
        for j in range(1, sizes[o][1]):
            send[p, j - 1] = piece[j * gz:(j + 1) * gz].astype(jnp.bfloat16)
            push(send.at[p, j - 1], recv.at[p, j - 1], send_sems.at[3 + o], sems2.at[t], hops[o][1](j))
        mine[t, :gz] = piece[:gz]

    def third(p):
        pieces = []
        for o in range(2):
            t = 2 * p + o
            recv = two[o][1]
            if sizes[o][1] > 1:
                arrived(recv.at[p], sems2.at[t])
            piece = mine[t, :gz]
            for j in range(1, sizes[o][1]):
                piece = piece + recv[p, j - 1].astype(jnp.float32)
            pieces.append(piece)
        for i in range(1, gz):
            s3[p, i - 1] = jnp.concatenate([piece[i:i + 1] for piece in pieces], axis=0).astype(jnp.bfloat16)
            push(s3.at[p, i - 1], r3.at[p, i - 1], send_sems.at[5], sems3.at[p], z_peer(i))
        own.append(jnp.concatenate([piece[0:1] for piece in pieces], axis=0))

    reach = small_send.shape[2] // 2
    stages = ((1, lambda j: sibling), (gx - 1, x_peer), (gy - 1, y_peer), (gz - 1, z_peer))

    def small_start():
        lane = lax.broadcasted_iota(jnp.int32, (rows, reach), 1).astype(jnp.float32)
        hits = jnp.where(lane == cls_col, 1.0, 0.0)
        small_send[0, :, :reach] = jnp.sum(hits, axis=0, keepdims=True)
        small_send[0, :, reach:] = jnp.sum(hits * sums["wedge"], axis=0, keepdims=True)
        small_push(0)

    def small_push(k):
        at = sum(n for n, _ in stages[:k])
        for j in range(stages[k][0]):
            push(small_send.at[k], small_recv.at[at + j], send_sems.at[6], small_sems.at[k], stages[k][1](j + 1))

    def small_take(k):
        at, n = sum(n for n, _ in stages[:k]), stages[k][0]
        tally = small_send[k]
        if n:
            arrived(small_recv.at[pl.ds(at, n)], small_sems.at[k])
        for j in range(n):
            tally = tally + small_recv[at + j]
        return tally

    def small_next(k):
        small_send[k + 1] = small_take(k)
        small_push(k + 1)

    def score():
        arrived(all_ref.at[pl.ds(half, half)], ag_sems.at[0])
        nt = (((1,), (1,)), ((), ()))
        group = min(classes, 32)
        out = jnp.zeros((rows, classes), jnp.float32)
        power = sums["power"]
        for g in range(classes // group):
            inter = jnp.zeros((rows, group), jnp.float32)
            energy = jnp.zeros((rows, group), jnp.float32)
            lines = slice(g * group, (g + 1) * group)
            for t in range(CHUNKS):
                width = max(0, min(span, coef - t * span))
                if width == 0:
                    continue
                cols = slice(t * span, t * span + width)
                both = jnp.swapaxes(all_ref[lines, :, cols].astype(jnp.float32), 0, 1)
                real, imag = both[0], both[1]
                ref_power = (real * real + imag * imag).astype(jnp.bfloat16)
                inter = inter + lax.dot_general(data[t, :, :width], real.astype(jnp.bfloat16), nt, preferred_element_type=jnp.float32)
                inter = inter + lax.dot_general(data[t, :, span:span + width], imag.astype(jnp.bfloat16), nt, preferred_element_type=jnp.float32)
                energy = energy + lax.dot_general(low[:, cols], ref_power, nt, preferred_element_type=jnp.float32)
            value = inter / (math.sqrt(coef) * jnp.sqrt((energy / coef + EPS) * (power / coef + EPS)))
            lane = lax.broadcasted_iota(jnp.int32, (group, classes), 1)
            place = jnp.where(ids[0][lines] == lane, 1.0, 0.0)
            out = out + jnp.dot(value, place, precision=lax.Precision.HIGHEST, preferred_element_type=jnp.float32)
        scores_ref[...] = out

    def means(p, floor):
        if gz > 1:
            arrived(r3.at[p], sems3.at[p])
        whole = own[p]
        for i in range(1, gz):
            whole = whole + r3[p, i - 1].astype(jnp.float32)
        scale = 1.0 / (whole[:, 2 * span:] + floor)
        for o in range(2):
            start = (2 * p + o) * span
            width = max(0, min(span, coef - start))
            for q in range(2):
                if width:
                    mean = whole[o:o + 1, q * span:q * span + width] * scale[o:o + 1, :width]
                    means_ref[0, q:q + 1, start:start + width] = mean

    compute(0)
    compute(1)
    pl.semaphore_wait(barrier, len(peers))
    cores(0)
    cores(1)
    ag_own()
    compute(2)
    compute(3)
    cores(2)
    cores(3)
    first(0)
    first(1)
    ag_forward(0, 1, 2)
    compute(4)
    compute(5)
    cores(4)
    cores(5)
    small_start()
    first(2)
    first(3)
    ag_core(0, 1, 2)
    first(4)
    first(5)
    ag_rest()
    small_next(0)
    second(0)
    second(1)
    small_next(1)
    second(2)
    second(3)
    third(0)
    small_next(2)
    second(4)
    second(5)
    third(1)
    ag_forward(1, gz - 1, 6)
    third(2)
    ag_core(1, gz - 1, 6)
    score()
    tally = small_take(3)
    load_ref[...] = tally[:, :classes] * classes / total
    lane = lax.broadcasted_iota(jnp.int32, (1, reach), 1)
    wedge_total = jnp.sum(jnp.where(lane == me, tally[:, reach:], 0.0), axis=1, keepdims=True)
    floor = TAU * (wedge_total / coef + 1.0)
    for p in range(PAIRS):
        means(p, floor)

    whole_of(all_ref.at[pl.ds(0, classes - 1)], ag_send_sem).wait_send()
    for ref, at in ((send_core, 0), (s1x, 1), (s1y, 2), (s2x, 3), (s2y, 4), (s3, 5), (small_recv, 6)):
        whole_of(ref, send_sems.at[at]).wait_send()


def finish(*arrays):
    n = len(arrays)

    def put(*refs):
        sems = refs[2 * n]
        copies = [pltpu.make_async_copy(refs[i], refs[n + i], sems.at[i]) for i in range(n)]
        for copy in copies:
            copy.start()
        for copy in copies:
            copy.wait()

    scores, means, load = pl.pallas_call(
        put,
        out_shape=tuple(jax.ShapeDtypeStruct(a.shape, a.dtype) for a in arrays),
        in_specs=[pl.BlockSpec(memory_space=pltpu.VMEM)] * n,
        out_specs=(pl.BlockSpec(memory_space=pltpu.HBM),) * n,
        scratch_shapes=[pltpu.SemaphoreType.DMA((n,))],
        compiler_params=pltpu.CompilerParams(vmem_limit_bytes=1024 * 1024),
    )(*arrays)
    return (scores, means, load[0])


def body(particles, references, assignment, orientation, tilt_range):
    part_rows = particles.shape[0]
    coef = particles.shape[2]
    devices = lax.axis_size("dom")
    classes = references.shape[0] * devices
    assert references.shape[0] == 1
    gx, gy, gz = factor(devices)
    total = part_rows * devices
    span = -(-coef // (CHUNKS * SUB)) * SUB
    padded = CHUNKS * span
    width = 2 * (-(-classes // LANES) * LANES)
    half = classes // 2

    vmem = pl.BlockSpec(memory_space=pltpu.VMEM)
    hbm = pl.BlockSpec(memory_space=pltpu.HBM)
    dma = pltpu.SemaphoreType.DMA
    bf16, f32, i32 = jnp.bfloat16, jnp.float32, jnp.int32
    wide = 3 * span

    def hop(n, lines):
        return [((PAIRS, max(1, n - 1), lines, wide), bf16)] * 2

    buffers = [
        ((part_rows, 2, coef), bf16),
        ((1, part_rows), i32),
        ((1, part_rows), i32),
        ((2, part_rows), i32),
        ((CHUNKS, part_rows, wide), bf16),
        ((part_rows, padded), bf16),
        ((classes, 2, coef), bf16),
        ((CHUNKS, half, wide), f32),
        ((CHUNKS, half, wide), bf16),
        ((CHUNKS, half, wide), bf16),
        *hop(gx, gy * gz), *hop(gy, gx * gz), *hop(gy, gz), *hop(gx, gz), *hop(gz, 2),
        ((4, 1, width), f32),
        ((gx + gy + gz - 2, 1, width), f32),
    ]
    held = sum(math.prod(shape) * jnp.dtype(kind).itemsize for shape, kind in buffers)
    limit = min(60, held // 2**20 + 8) * 2**20
    scores, means, load = pl.pallas_call(
        functools.partial(kernel, gx, gy, gz, span, coef, total),
        out_shape=(
            jax.ShapeDtypeStruct((part_rows, classes), f32),
            jax.ShapeDtypeStruct((1, 2, coef), f32),
            jax.ShapeDtypeStruct((1, classes), f32),
        ),
        in_specs=[hbm] * 5,
        out_specs=(vmem, vmem, vmem),
        scratch_shapes=[pltpu.VMEM(shape, kind) for shape, kind in buffers] + [
            dma((4 + PAIRS,)), dma((10,)), dma, dma((CHUNKS,)), dma((CHUNKS,)), dma((CHUNKS,)), dma((PAIRS,)),
            dma((4,)), dma((7,)),
        ],
        compiler_params=pltpu.CompilerParams(
            collective_id=0, has_side_effects=True, vmem_limit_bytes=limit
        ),
    )(*[
        pltpu.with_memory_space_constraint(v, pltpu.HBM)
        for v in (particles, references, assignment.reshape(1, part_rows), orientation[None, :], tilt_range)
    ])
    return finish(scores, means, load)


def solution(mesh):
    in_specs = (
        P("dom", None, None),
        P("dom", None, None),
        P("dom", None),
        P("dom"),
        P(None, "dom"),
    )
    out_specs = (P("dom", None), P("dom", None, None), P())
    return jax.shard_map(body, mesh=mesh, in_specs=in_specs, out_specs=out_specs, check_vma=False)
```

```python
import functools
import math

import jax
import jax.numpy as jnp
from jax import lax
from jax.experimental import pallas as pl
from jax.experimental.pallas import tpu as pltpu
from jax.sharding import PartitionSpec as P

GRID = 24
ORIENTS = 36
EPS = 1e-06
GAIN = 6.0
TAU = 0.5
LANES = 128
MESH = pl.DeviceIdType.MESH

PAIRS = 3
CHUNKS = 2 * PAIRS
SUB = 640
ORDERS = ("xzy", "yzx", "xyz", "yxz", "xyz", "yxz")
SMALL = "xyz"


def factor(devices):
    chips = devices // 2
    log = chips.bit_length() - 1
    gx = 1 << (log // 3)
    gy = 1 << ((log - log // 3) // 2)
    return gx, gy, chips // (gx * gy)


def column(row):
    rows = row.shape[1]
    line = lax.broadcasted_iota(jnp.int32, (rows, rows), 0)
    lane = lax.broadcasted_iota(jnp.int32, (rows, rows), 1)
    return jnp.sum(jnp.where(line == lane, row, 0.0), axis=1, keepdims=True)


def frequencies(first, width):
    index = (lax.broadcasted_iota(jnp.int32, (1, width), 1) + first).astype(jnp.float32)
    plane = jnp.floor((index + 0.5) * (1.0 / (GRID * GRID)))
    rest = index - plane * (GRID * GRID)
    col_x = jnp.floor((rest + 0.5) * (1.0 / GRID))
    col_z = rest - col_x * GRID
    freq_x = jnp.where(col_x >= GRID // 2, col_x - GRID, col_x)
    freq_z = jnp.where(col_z >= GRID // 2, col_z - GRID, col_z)
    return freq_x, plane, freq_z, index


def kernel(
    gx, gy, gz, span, coef, total,
    part_hbm, ref_hbm, cls_hbm, orient_hbm, tilt_hbm,
    scores_ref, means_ref, load_ref,
    part, cls_ref, orient_ref, tilt_ref,
    data, low, all_ref, mine, send_core, recv_core, small_send, small_recv, *rest,
):
    hop_sends, hop_recvs = rest[:3 * CHUNKS], rest[3 * CHUNKS:6 * CHUNKS]
    in_sems, ag_sems, core_sems, hop_sems, small_sems, send_sems = rest[6 * CHUNKS:]
    me = lax.axis_index("dom")
    core = lax.rem(me, 2)
    chip = me // 2
    x = lax.rem(chip, gx)
    y = lax.rem(chip // gx, gy)
    z = chip // (gx * gy)
    sibling = me + 1 - 2 * core
    classes = 2 * gx * gy * gz
    half = classes // 2
    rows = part.shape[0]
    wide = 3 * span
    cut = coef // 2 // LANES * LANES

    def device(x_at, y_at, z_at, c_at):
        return ((z_at * gy + y_at) * gx + x_at) * 2 + c_at

    def x_peer(j):
        return device(lax.rem(x + j, gx), y, z, core)

    def y_peer(j):
        return device(x, lax.rem(y + j, gy), z, core)

    def z_peer(j):
        return device(x, y, lax.rem(z + j, gz), core)

    sizes = {"x": gx, "y": gy, "z": gz}
    peer_of = {"x": x_peer, "y": y_peer, "z": z_peer}

    def fetch(src, dst, at):
        copy = pltpu.make_async_copy(src, dst, in_sems.at[at])
        copy.start()
        return copy

    barrier = pltpu.get_barrier_semaphore()
    peers = [sibling]
    peers += [x_peer(j) for j in range(1, gx)]
    peers += [y_peer(j) for j in range(1, gy)]
    peers += [z_peer(j) for j in range(1, gz)]
    for peer in peers:
        pl.semaphore_signal(barrier, inc=1, device_id=(peer,), device_id_type=MESH)
    own_ref = fetch(ref_hbm.at[0], all_ref.at[0], 0)
    metas = [
        fetch(orient_hbm, orient_ref, 1),
        fetch(tilt_hbm, tilt_ref, 2),
        fetch(cls_hbm, cls_ref, 3),
    ]
    part_copies = []
    for p in range(PAIRS):
        first = 2 * p * span
        cols = pl.ds(first, min(2 * span, coef - first))
        part_copies.append(fetch(part_hbm.at[:, :, cols], part.at[:, :, cols], 4 + p))

    def push(src, dst, send_sem, recv_sem, target):
        pltpu.make_async_remote_copy(
            src_ref=src, dst_ref=dst, send_sem=send_sem, recv_sem=recv_sem,
            device_id=(target,), device_id_type=MESH,
        ).start()

    def whole_of(ref, sem):
        return pltpu.make_async_remote_copy(
            src_ref=ref, dst_ref=ref, send_sem=sem, recv_sem=sem,
            device_id=(sibling,), device_id_type=MESH,
        )

    def arrived(ref, sem):
        whole_of(ref, sem).wait_recv()

    def slot(dx, dy, dc):
        return ((dc * gx + dx) * gy + dy) * gz

    def give(src_slot, dst_slot, n, lanes, at, target):
        src = all_ref.at[pl.ds(src_slot, n), :, lanes]
        dst = all_ref.at[pl.ds(dst_slot, n), :, lanes]
        push(src, dst, send_sems.at[0], ag_sems.at[at], target)

    every = slice(0, coef)
    front, back = slice(0, cut), slice(cut, coef)

    def ag_direct(at, n, sem):
        for j in range(1, gx):
            give(at, slot(gx - j, 0, 0) + at, n, every, sem, x_peer(j))
        for j in range(1, gy):
            give(at, slot(0, gy - j, 0) + at, n, every, sem + 1, y_peer(j))
        give(at, slot(0, 0, 1) + at, n, every, 0, sibling)

    def ag_forward(at, n, sem):
        if gx > 1:
            arrived(all_ref.at[pl.ds(0, (gx - 1) * n)], ag_sems.at[sem])
        for dx in range(1, gx):
            for j in range(1, gy):
                give(slot(dx, 0, 0) + at, slot(dx, gy - j, 0) + at, n, front, sem + 2, y_peer(j))
        if gy > 1:
            arrived(all_ref.at[pl.ds(0, (gy - 1) * n)], ag_sems.at[sem + 1])
        for dy in range(1, gy):
            for j in range(1, gx):
                give(slot(0, dy, 0) + at, slot(gx - j, dy, 0) + at, n, back, sem + 3, x_peer(j))
        for dx in range(1, gx):
            give(slot(dx, 0, 0) + at, slot(dx, 0, 1) + at, n, every, 0, sibling)
        for dy in range(1, gy):
            give(slot(0, dy, 0) + at, slot(0, dy, 1) + at, n, every, 0, sibling)

    def ag_core(at, n, sem):
        count = (gx - 1) * (gy - 1) * n
        if count:
            arrived(all_ref.at[pl.ds(0, count), :, front], ag_sems.at[sem + 2])
            arrived(all_ref.at[pl.ds(0, count), :, back], ag_sems.at[sem + 3])
        for dx in range(1, gx):
            for dy in range(1, gy):
                give(slot(dx, dy, 0) + at, slot(dx, dy, 1) + at, n, every, 0, sibling)

    def ag_own():
        own_ref.wait()
        for j in range(1, gz):
            give(0, gz - j, 1, every, 1, z_peer(j))
        ag_direct(0, 1, 2)

    def ag_rest():
        arrived(all_ref.at[pl.ds(1, gz - 1)], ag_sems.at[1])
        ag_direct(1, gz - 1, 6)

    for copy in metas:
        copy.wait()
    angle = orient_ref[...].astype(jnp.float32) * (2.0 * math.pi / ORIENTS)
    bins = tilt_ref[...].astype(jnp.float32)
    low_end = -(40.0 + 1.5 * bins[0:1]) * (math.pi / 180.0)
    high_end = (40.0 + 1.5 * bins[1:2]) * (math.pi / 180.0)
    sin_a, cos_a = column(jnp.sin(angle)), column(jnp.cos(angle))
    cos_c = column(jnp.cos(low_end + high_end))
    sin_c = column(jnp.sin(low_end + high_end))
    cos_w = column(jnp.cos(high_end - low_end))
    cls_row = cls_ref[...].astype(jnp.float32)
    cls_col = column(cls_row)

    def log2(n):
        return n.bit_length() - 1

    row = lax.broadcasted_iota(jnp.int32, (classes, 1), 0)

    def ids_of(order):
        left, at = row, {}
        for dim in reversed(order):
            at[dim] = left & (sizes[dim] - 1)
            left = lax.shift_right_logical(left, log2(sizes[dim]))
        return device((at["x"] + x) & (gx - 1), (at["y"] + y) & (gy - 1), (at["z"] + z) & (gz - 1), (left + core) & 1)

    ids = ids_of("xyz")
    onehot = {}
    for order in ORDERS:
        if order not in onehot:
            onehot[order] = jnp.where(ids_of(order).astype(jnp.float32) == cls_row, 1.0, 0.0).astype(jnp.bfloat16)
    sums = {"wedge": jnp.zeros((rows, 1), jnp.float32), "power": jnp.zeros((rows, 1), jnp.float32)}

    def parts(first):
        width = max(0, min(SUB, coef - first))
        pieces = []
        if width:
            both = part[:, :, first:first + width].astype(jnp.float32)
            pieces.append(jnp.swapaxes(both, 0, 1))
        if width < SUB:
            pieces.append(jnp.zeros((2, rows, SUB - width), jnp.float32))
        both = jnp.concatenate(pieces, axis=2) if len(pieces) > 1 else pieces[0]
        return both[0], both[1]

    def compute(t):
        if t % 2 == 0:
            part_copies[t // 2].wait()
        for s in range(span // SUB):
            first = t * span + s * SUB
            freq_x, freq_y, freq_z, index = frequencies(first, SUB)
            along = freq_y * cos_a - freq_x * sin_a
            along_sq = along * along
            z_sq = freq_z * freq_z
            scale = 1.0 / (along_sq + (z_sq + 1.0))
            value = ((along_sq - z_sq) * cos_c - (2.0 * along * freq_z) * sin_c) * scale - cos_w
            wedge = 1.0 / (1.0 + jnp.exp(value * (-GAIN)))
            real, imag = parts(first)
            sums["power"] = sums["power"] + jnp.sum(wedge * (real * real + imag * imag), axis=1, keepdims=True)
            inside = wedge if first + SUB <= coef else jnp.where(index < coef, wedge, 0.0)
            sums["wedge"] = sums["wedge"] + jnp.sum(inside, axis=1, keepdims=True)
            at = s * SUB
            data[t, :, at:at + SUB] = (wedge * real).astype(jnp.bfloat16)
            data[t, :, span + at:span + at + SUB] = (wedge * imag).astype(jnp.bfloat16)
            data[t, :, 2 * span + at:2 * span + at + SUB] = (wedge * wedge).astype(jnp.bfloat16)
            low[:, first:first + SUB] = wedge.astype(jnp.bfloat16)
        for q in range(3):
            cols = slice(q * span, (q + 1) * span)
            both = jnp.dot(onehot[ORDERS[t]], data[t, :, cols], preferred_element_type=jnp.float32)
            send_core[t, :, cols] = both[half:].astype(jnp.bfloat16)
            mine[t, :, cols] = both[:half]

    def cores(t):
        push(send_core.at[t], recv_core.at[t], send_sems.at[1], core_sems.at[t], sibling)

    def fold(line):
        return jnp.concatenate([line[:, :wide // 2], line[:, wide // 2:]], axis=0)

    def taken(t, k):
        if k < 0:
            arrived(recv_core.at[t], core_sems.at[t])
            return mine[t] + recv_core[t].astype(jnp.float32)
        n = sizes[ORDERS[t][k]]
        lines = math.prod(sizes[dim] for dim in ORDERS[t][k + 1:])
        piece = mine[t, :lines]
        if lines == 1:
            piece = fold(piece)
        recv = hop_recvs[3 * t + k]
        if n > 1:
            arrived(recv, hop_sems.at[3 * t + k])
        for j in range(1, n):
            piece = piece + recv[j - 1].astype(jnp.float32)
        return piece

    def hop(t, k):
        dim = ORDERS[t][k]
        lines = math.prod(sizes[dim] for dim in ORDERS[t][k + 1:])
        piece = taken(t, k - 1)
        send, recv = hop_sends[3 * t + k], hop_recvs[3 * t + k]
        for j in range(1, sizes[dim]):
            part_of = piece[j * lines:(j + 1) * lines]
            if lines == 1:
                part_of = fold(part_of)
            send[j - 1] = part_of.astype(jnp.bfloat16)
            push(send.at[j - 1], recv.at[j - 1], send_sems.at[2], hop_sems.at[3 * t + k], peer_of[dim](j))
        mine[t, :lines] = piece[:lines]

    def first(t):
        hop(t, 0)

    def second(t):
        hop(t, 1)

    def third(t):
        hop(t, 2)

    reach = small_send.shape[2] // 2
    stages = [(1, lambda j: sibling)] + [(sizes[dim] - 1, peer_of[dim]) for dim in SMALL]

    def small_start():
        lane = lax.broadcasted_iota(jnp.int32, (rows, reach), 1).astype(jnp.float32)
        hits = jnp.where(lane == cls_col, 1.0, 0.0)
        small_send[0, :, :reach] = jnp.sum(hits, axis=0, keepdims=True)
        small_send[0, :, reach:] = jnp.sum(hits * sums["wedge"], axis=0, keepdims=True)
        small_push(0)

    def small_push(k):
        at = sum(n for n, _ in stages[:k])
        for j in range(stages[k][0]):
            push(small_send.at[k], small_recv.at[at + j], send_sems.at[3], small_sems.at[k], stages[k][1](j + 1))

    def small_take(k):
        at, n = sum(n for n, _ in stages[:k]), stages[k][0]
        tally = small_send[k]
        if n:
            arrived(small_recv.at[pl.ds(at, n)], small_sems.at[k])
        for j in range(n):
            tally = tally + small_recv[at + j]
        return tally

    def small_next(k):
        small_send[k + 1] = small_take(k)
        small_push(k + 1)

    def score():
        arrived(all_ref.at[pl.ds(half, half)], ag_sems.at[0])
        nt = (((1,), (1,)), ((), ()))
        group = min(classes, 32)
        out = jnp.zeros((rows, classes), jnp.float32)
        power = sums["power"]
        for g in range(classes // group):
            inter = jnp.zeros((rows, group), jnp.float32)
            energy = jnp.zeros((rows, group), jnp.float32)
            lines = slice(g * group, (g + 1) * group)
            for t in range(CHUNKS):
                width = max(0, min(span, coef - t * span))
                if width == 0:
                    continue
                cols = slice(t * span, t * span + width)
                both = jnp.swapaxes(all_ref[lines, :, cols].astype(jnp.float32), 0, 1)
                real, imag = both[0], both[1]
                ref_power = (real * real + imag * imag).astype(jnp.bfloat16)
                inter = inter + lax.dot_general(data[t, :, :width], real.astype(jnp.bfloat16), nt, preferred_element_type=jnp.float32)
                inter = inter + lax.dot_general(data[t, :, span:span + width], imag.astype(jnp.bfloat16), nt, preferred_element_type=jnp.float32)
                energy = energy + lax.dot_general(low[:, cols], ref_power, nt, preferred_element_type=jnp.float32)
            value = inter / (math.sqrt(coef) * jnp.sqrt((energy / coef + EPS) * (power / coef + EPS)))
            lane = lax.broadcasted_iota(jnp.int32, (group, classes), 1)
            place = jnp.where(ids[lines] == lane, 1.0, 0.0)
            out = out + jnp.dot(value, place, precision=lax.Precision.HIGHEST, preferred_element_type=jnp.float32)
        scores_ref[...] = out

    def means(t, floor):
        whole = taken(t, 2)
        flat = jnp.concatenate([whole[0:1], whole[1:2]], axis=1)
        start = t * span
        width = max(0, min(span, coef - start))
        if width == 0:
            return
        scale = 1.0 / (flat[:, 2 * span:2 * span + width] + floor)
        for q in range(2):
            means_ref[0, q:q + 1, start:start + width] = flat[:, q * span:q * span + width] * scale

    compute(0)
    pl.semaphore_wait(barrier, len(peers))
    ag_own()
    cores(0)
    compute(1)
    cores(1)
    compute(2)
    cores(2)
    compute(3)
    cores(3)
    hop(0, 0)
    hop(1, 0)
    compute(4)
    cores(4)
    compute(5)
    cores(5)
    small_start()
    hop(2, 0)
    hop(3, 0)
    ag_forward(0, 1, 2)
    hop(4, 0)
    hop(5, 0)
    small_next(0)
    hop(0, 1)
    hop(1, 1)
    ag_rest()
    ag_core(0, 1, 2)
    hop(2, 1)
    hop(3, 1)
    hop(4, 1)
    hop(5, 1)
    small_next(1)
    hop(0, 2)
    hop(1, 2)
    ag_forward(1, gz - 1, 6)
    hop(2, 2)
    hop(3, 2)
    hop(4, 2)
    hop(5, 2)
    small_next(2)
    ag_core(1, gz - 1, 6)
    score()
    tally = small_take(3)
    load_ref[...] = tally[:, :classes] * classes / total
    lane = lax.broadcasted_iota(jnp.int32, (1, reach), 1)
    wedge_total = jnp.sum(jnp.where(lane == me, tally[:, reach:], 0.0), axis=1, keepdims=True)
    floor = TAU * (wedge_total / coef + 1.0)
    for t in range(CHUNKS):
        means(t, floor)

    whole_of(all_ref.at[pl.ds(0, classes - 1)], send_sems.at[0]).wait_send()
    whole_of(send_core, send_sems.at[1]).wait_send()
    whole_of(all_ref.at[pl.ds(0, classes - 2), :, :CHUNKS * wide // 4], send_sems.at[2]).wait_send()
    whole_of(small_recv, send_sems.at[3]).wait_send()


def finish(*arrays):
    n = len(arrays)

    def put(*refs):
        sems = refs[2 * n]
        copies = [pltpu.make_async_copy(refs[i], refs[n + i], sems.at[i]) for i in range(n)]
        for copy in copies:
            copy.start()
        for copy in copies:
            copy.wait()

    scores, means, load = pl.pallas_call(
        put,
        out_shape=tuple(jax.ShapeDtypeStruct(a.shape, a.dtype) for a in arrays),
        in_specs=[pl.BlockSpec(memory_space=pltpu.VMEM)] * n,
        out_specs=(pl.BlockSpec(memory_space=pltpu.HBM),) * n,
        scratch_shapes=[pltpu.SemaphoreType.DMA((n,))],
        compiler_params=pltpu.CompilerParams(vmem_limit_bytes=1024 * 1024),
    )(*arrays)
    return (scores, means, load[0])


def body(particles, references, assignment, orientation, tilt_range):
    part_rows = particles.shape[0]
    coef = particles.shape[2]
    devices = lax.axis_size("dom")
    classes = references.shape[0] * devices
    assert references.shape[0] == 1
    gx, gy, gz = factor(devices)
    total = part_rows * devices
    span = -(-coef // (CHUNKS * SUB)) * SUB
    padded = CHUNKS * span
    width = 2 * (-(-classes // LANES) * LANES)
    half = classes // 2

    vmem = pl.BlockSpec(memory_space=pltpu.VMEM)
    hbm = pl.BlockSpec(memory_space=pltpu.HBM)
    dma = pltpu.SemaphoreType.DMA
    bf16, f32, i32 = jnp.bfloat16, jnp.float32, jnp.int32
    wide = 3 * span

    sizes = {"x": gx, "y": gy, "z": gz}
    hops = []
    for order in ORDERS:
        for k, dim in enumerate(order):
            lines = math.prod(sizes[d] for d in order[k + 1:])
            shape = (lines, wide) if lines > 1 else (2, wide // 2)
            hops.append(((max(1, sizes[dim] - 1), *shape), bf16))
    buffers = [
        ((part_rows, 2, coef), bf16),
        ((1, part_rows), i32),
        ((1, part_rows), i32),
        ((2, part_rows), i32),
        ((CHUNKS, part_rows, wide), bf16),
        ((part_rows, padded), bf16),
        ((classes, 2, coef), bf16),
        ((CHUNKS, half, wide), f32),
        ((CHUNKS, half, wide), bf16),
        ((CHUNKS, half, wide), bf16),
        ((4, 1, width), f32),
        ((gx + gy + gz - 2, 1, width), f32),
        *hops, *hops,
    ]
    held = sum(math.prod(shape) * jnp.dtype(kind).itemsize for shape, kind in buffers)
    limit = min(60, held // 2**20 + 8) * 2**20
    scores, means, load = pl.pallas_call(
        functools.partial(kernel, gx, gy, gz, span, coef, total),
        out_shape=(
            jax.ShapeDtypeStruct((part_rows, classes), f32),
            jax.ShapeDtypeStruct((1, 2, coef), f32),
            jax.ShapeDtypeStruct((1, classes), f32),
        ),
        in_specs=[hbm] * 5,
        out_specs=(vmem, vmem, vmem),
        scratch_shapes=[pltpu.VMEM(shape, kind) for shape, kind in buffers] + [
            dma((4 + PAIRS,)), dma((10,)), dma((CHUNKS,)), dma((3 * CHUNKS,)), dma((4,)), dma((4,)),
        ],
        compiler_params=pltpu.CompilerParams(
            collective_id=0, has_side_effects=True, vmem_limit_bytes=limit
        ),
    )(*[
        pltpu.with_memory_space_constraint(v, pltpu.HBM)
        for v in (particles, references, assignment.reshape(1, part_rows), orientation[None, :], tilt_range)
    ])
    return finish(scores, means, load)


def solution(mesh):
    in_specs = (
        P("dom", None, None),
        P("dom", None, None),
        P("dom", None),
        P("dom"),
        P(None, "dom"),
    )
    out_specs = (P("dom", None), P("dom", None, None), P())
    return jax.shard_map(body, mesh=mesh, in_specs=in_specs, out_specs=out_specs, check_vma=False)
```

```python
import functools
import math

import jax
import jax.numpy as jnp
from jax import lax
from jax.experimental import pallas as pl
from jax.experimental.pallas import tpu as pltpu
from jax.sharding import PartitionSpec as P

GRID = 24
ORIENTS = 36
EPS = 1e-06
GAIN = 6.0
TAU = 0.5
LANES = 128
MESH = pl.DeviceIdType.MESH

SHARES = (10, 10, 10, 10, 10, 10)
CHUNKS = len(SHARES)
SUB = 640
ORDERS = ("xzy", "yzx", "xyz", "yxz", "xyz", "yxz")
SMALL = "xyz"
PIECES = 3


def factor(devices):
    chips = devices // 2
    log = chips.bit_length() - 1
    gx = 1 << (log // 3)
    gy = 1 << ((log - log // 3) // 2)
    return gx, gy, chips // (gx * gy)


def spans_of(coef):
    unit = sum(SHARES)
    pairs = -(-coef // (4 * LANES)) * 2
    ends = [sum(SHARES[:t + 1]) * pairs // unit for t in range(CHUNKS)]
    return [(end - start) * 2 * LANES for start, end in zip([0] + ends, ends)]


def column(row):
    rows = row.shape[1]
    line = lax.broadcasted_iota(jnp.int32, (rows, rows), 0)
    lane = lax.broadcasted_iota(jnp.int32, (rows, rows), 1)
    return jnp.sum(jnp.where(line == lane, row, 0.0), axis=1, keepdims=True)


def frequencies(first, width):
    index = (lax.broadcasted_iota(jnp.int32, (1, width), 1) + first).astype(jnp.float32)
    plane = jnp.floor((index + 0.5) * (1.0 / (GRID * GRID)))
    rest = index - plane * (GRID * GRID)
    col_x = jnp.floor((rest + 0.5) * (1.0 / GRID))
    col_z = rest - col_x * GRID
    freq_x = jnp.where(col_x >= GRID // 2, col_x - GRID, col_x)
    freq_z = jnp.where(col_z >= GRID // 2, col_z - GRID, col_z)
    return freq_x, plane, freq_z, index


def kernel(
    gx, gy, gz, spans, coef, total,
    part_hbm, ref_hbm, cls_hbm, orient_hbm, tilt_hbm,
    scores_ref, means_ref, load_ref,
    part, cls_ref, orient_ref, tilt_ref,
    low, all_ref, ready, small_send, small_recv, *rest,
):
    hop_sends, hop_recvs = rest[:3 * CHUNKS], rest[3 * CHUNKS:6 * CHUNKS]
    data, mine, send_core, recv_core = (rest[k * CHUNKS:(k + 1) * CHUNKS] for k in range(6, 10))
    in_sems, ag_sems, core_sems, hop_sems, small_sems, send_sems = rest[10 * CHUNKS:]
    starts = [sum(spans[:t]) for t in range(CHUNKS)]
    widths = [max(0, min(spans[t], coef - starts[t])) for t in range(CHUNKS)]
    me = lax.axis_index("dom")
    core = lax.rem(me, 2)
    chip = me // 2
    x = lax.rem(chip, gx)
    y = lax.rem(chip // gx, gy)
    z = chip // (gx * gy)
    sibling = me + 1 - 2 * core
    classes = 2 * gx * gy * gz
    half = classes // 2
    rows = part.shape[0]
    cut = coef // 2 // LANES * LANES

    def device(x_at, y_at, z_at, c_at):
        return ((z_at * gy + y_at) * gx + x_at) * 2 + c_at

    def x_peer(j):
        return device(lax.rem(x + j, gx), y, z, core)

    def y_peer(j):
        return device(x, lax.rem(y + j, gy), z, core)

    def x_cross(j):
        return device(lax.rem(x + j, gx), y, z, 1 - core)

    def y_cross(j):
        return device(x, lax.rem(y + j, gy), z, 1 - core)

    def z_peer(j):
        return device(x, y, lax.rem(z + j, gz), core)

    sizes = {"x": gx, "y": gy, "z": gz}
    peer_of = {"x": x_peer, "y": y_peer, "z": z_peer}

    def fetch(src, dst, at):
        copy = pltpu.make_async_copy(src, dst, in_sems.at[at])
        copy.start()
        return copy

    barrier = pltpu.get_barrier_semaphore()
    peers = [sibling]
    peers += [x_peer(j) for j in range(1, gx)]
    peers += [y_peer(j) for j in range(1, gy)]
    peers += [z_peer(j) for j in range(1, gz)]
    peers += [x_cross(j) for j in range(1, gx)]
    peers += [y_cross(j) for j in range(1, gy)]
    for peer in peers:
        pl.semaphore_signal(barrier, inc=1, device_id=(peer,), device_id_type=MESH)
    metas = [
        fetch(orient_hbm, orient_ref, 1),
        fetch(tilt_hbm, tilt_ref, 2),
        fetch(cls_hbm, cls_ref, 3),
    ]
    own_ref = fetch(ref_hbm.at[0], all_ref.at[0], 0)
    part_copies = []
    for t in range(CHUNKS):
        cols = pl.ds(starts[t], widths[t])
        part_copies.append(fetch(part_hbm.at[:, :, cols], part.at[:, :, cols], 4 + t))

    def push(src, dst, send_sem, recv_sem, target):
        pltpu.make_async_remote_copy(
            src_ref=src, dst_ref=dst, send_sem=send_sem, recv_sem=recv_sem,
            device_id=(target,), device_id_type=MESH,
        ).start()

    def whole_of(ref, sem):
        return pltpu.make_async_remote_copy(
            src_ref=ref, dst_ref=ref, send_sem=sem, recv_sem=sem,
            device_id=(sibling,), device_id_type=MESH,
        )

    def arrived(ref, sem):
        whole_of(ref, sem).wait_recv()

    def slot(dx, dy, dc):
        return ((dc * gx + dx) * gy + dy) * gz

    def give(src_slot, dst_slot, n, lanes, at, target):
        src = all_ref.at[pl.ds(src_slot, n), :, lanes]
        dst = all_ref.at[pl.ds(dst_slot, n), :, lanes]
        push(src, dst, send_sems.at[0], ag_sems.at[at], target)

    every = slice(0, coef)
    front, back = slice(0, cut), slice(cut, coef)

    def split(g):
        return 1 + g * (gz - 1) // PIECES, 1 + (g + 1) * (gz - 1) // PIECES

    def sem_of(g):
        return 3 + 4 * (g + 1)

    cross = sem_of(PIECES)

    def ag_direct(g):
        at, end = split(g) if g >= 0 else (0, 1)
        sem = sem_of(g)
        if at == end:
            return
        for j in range(1, gx):
            give(at, slot(gx - j, 0, 0) + at, end - at, every, sem, x_peer(j))
        for j in range(1, gy):
            give(at, slot(0, gy - j, 0) + at, end - at, every, sem + 1, y_peer(j))
        give(at, slot(0, 0, 1) + at, end - at, every, 0, sibling)

    def ag_forward(g):
        at, end = split(g) if g >= 0 else (0, 1)
        n, sem = end - at, sem_of(g)
        if n == 0:
            return
        if gx > 1:
            arrived(all_ref.at[pl.ds(0, (gx - 1) * n)], ag_sems.at[sem])
        for dx in range(1, gx):
            for j in range(1, gy):
                give(slot(dx, 0, 0) + at, slot(dx, gy - j, 0) + at, n, front, sem + 2, y_peer(j))
                if g == PIECES - 1:
                    give(slot(dx, 0, 0) + at, slot(dx, gy - j, 1) + at, n, front, cross, y_cross(j))
        if gy > 1:
            arrived(all_ref.at[pl.ds(0, (gy - 1) * n)], ag_sems.at[sem + 1])
        for dy in range(1, gy):
            for j in range(1, gx):
                give(slot(0, dy, 0) + at, slot(gx - j, dy, 0) + at, n, back, sem + 3, x_peer(j))
                if g == PIECES - 1:
                    give(slot(0, dy, 0) + at, slot(gx - j, dy, 1) + at, n, back, cross + 1, x_cross(j))
        for dx in range(1, gx):
            give(slot(dx, 0, 0) + at, slot(dx, 0, 1) + at, n, every, 0, sibling)
        for dy in range(1, gy):
            give(slot(0, dy, 0) + at, slot(0, dy, 1) + at, n, every, 0, sibling)

    def ag_core(g):
        at, end = split(g) if g >= 0 else (0, 1)
        n, sem = end - at, sem_of(g)
        count = (gx - 1) * (gy - 1) * n
        if count:
            arrived(all_ref.at[pl.ds(0, count), :, front], ag_sems.at[sem + 2])
            arrived(all_ref.at[pl.ds(0, count), :, back], ag_sems.at[sem + 3])
        if g == PIECES - 1:
            return
        for dx in range(1, gx):
            for dy in range(1, gy):
                give(slot(dx, dy, 0) + at, slot(dx, dy, 1) + at, n, every, 1, sibling)

    def ag_own():
        own_ref.wait()
        for j in range(1, gz):
            give(0, gz - j, 1, every, 2, z_peer(j))
        ag_direct(-1)

    def ag_z():
        if gz > 1:
            arrived(all_ref.at[pl.ds(1, gz - 1)], ag_sems.at[2])

    diag = (gx - 1) * (gy - 1) * gz
    early, late = [], []
    for dc in range(2):
        for dx in range(gx):
            for dy in range(gy):
                runs = late if dx and dy else early
                at = slot(dx, dy, dc)
                if runs and runs[-1][1] == at and at != half:
                    runs[-1] = (runs[-1][0], at + gz)
                else:
                    runs.append((at, at + gz))

    for copy in metas:
        copy.wait()
    angle = orient_ref[...].astype(jnp.float32) * (2.0 * math.pi / ORIENTS)
    bins = tilt_ref[...].astype(jnp.float32)
    low_end = -(40.0 + 1.5 * bins[0:1]) * (math.pi / 180.0)
    high_end = (40.0 + 1.5 * bins[1:2]) * (math.pi / 180.0)
    sin_a, cos_a = column(jnp.sin(angle)), column(jnp.cos(angle))
    cos_c = column(jnp.cos(low_end + high_end))
    sin_c = column(jnp.sin(low_end + high_end))
    cos_w = column(jnp.cos(high_end - low_end))
    cls_row = cls_ref[...].astype(jnp.float32)
    cls_col = column(cls_row)

    def log2(n):
        return n.bit_length() - 1

    row = lax.broadcasted_iota(jnp.int32, (classes, 1), 0)

    def ids_of(order):
        left, at = row, {}
        for dim in reversed(order):
            at[dim] = left & (sizes[dim] - 1)
            left = lax.shift_right_logical(left, log2(sizes[dim]))
        return device((at["x"] + x) & (gx - 1), (at["y"] + y) & (gy - 1), (at["z"] + z) & (gz - 1), (left + core) & 1)

    ids = ids_of("xyz")
    onehot = {}
    for order in ORDERS:
        if order not in onehot:
            onehot[order] = jnp.where(ids_of(order).astype(jnp.float32) == cls_row, 1.0, 0.0).astype(jnp.bfloat16)
    sums = {"wedge": jnp.zeros((rows, 1), jnp.float32), "power": jnp.zeros((rows, 1), jnp.float32)}

    def parts(first, size):
        width = max(0, min(size, coef - first))
        pieces = []
        if width:
            both = part[:, :, first:first + width].astype(jnp.float32)
            pieces.append(jnp.swapaxes(both, 0, 1))
        if width < size:
            pieces.append(jnp.zeros((2, rows, size - width), jnp.float32))
        both = jnp.concatenate(pieces, axis=2) if len(pieces) > 1 else pieces[0]
        return both[0], both[1]

    def wedges(first, size):
        freq_x, freq_y, freq_z, index = frequencies(first, size)
        along = freq_y * cos_a - freq_x * sin_a
        along_sq = along * along
        z_sq = freq_z * freq_z
        scale = 1.0 / (along_sq + (z_sq + 1.0))
        value = ((along_sq - z_sq) * cos_c - (2.0 * along * freq_z) * sin_c) * scale - cos_w
        wedge = 1.0 / (1.0 + jnp.exp(value * (-GAIN)))
        inside = wedge if first + size <= coef else jnp.where(index < coef, wedge, 0.0)
        sums["wedge"] = sums["wedge"] + jnp.sum(inside, axis=1, keepdims=True)
        return wedge

    def compute(t):
        span = spans[t]
        part_copies[t].wait()
        for at in range(0, span, SUB):
            first = starts[t] + at
            size = min(SUB, span - at)
            wedge = wedges(first, size)
            real, imag = parts(first, size)
            sums["power"] = sums["power"] + jnp.sum(wedge * (real * real + imag * imag), axis=1, keepdims=True)
            data[t][:, at:at + size] = (wedge * real).astype(jnp.bfloat16)
            data[t][:, span + at:span + at + size] = (wedge * imag).astype(jnp.bfloat16)
            data[t][:, 2 * span + at:2 * span + at + size] = (wedge * wedge).astype(jnp.bfloat16)
            low[:, first:first + size] = wedge.astype(jnp.bfloat16)
        for q in range(3):
            cols = slice(q * span, (q + 1) * span)
            both = jnp.dot(onehot[ORDERS[t]], data[t][:, cols], preferred_element_type=jnp.float32)
            send_core[t][:, cols] = both[half:].astype(jnp.bfloat16)
            mine[t][:, cols] = both[:half]

    def cores(t):
        push(send_core[t], recv_core[t], send_sems.at[1], core_sems.at[t], sibling)

    def fold(line):
        wide = line.shape[1]
        return jnp.concatenate([line[:, :wide // 2], line[:, wide // 2:]], axis=0)

    def taken(t, k):
        if k < 0:
            arrived(recv_core[t], core_sems.at[t])
            return mine[t][...] + recv_core[t][...].astype(jnp.float32)
        n = sizes[ORDERS[t][k]]
        lines = math.prod(sizes[dim] for dim in ORDERS[t][k + 1:])
        piece = mine[t][:lines]
        if lines == 1:
            piece = fold(piece)
        recv = hop_recvs[3 * t + k]
        if n > 1:
            arrived(recv, hop_sems.at[3 * t + k])
        for j in range(1, n):
            piece = piece + recv[j - 1].astype(jnp.float32)
        return piece

    def hop(t, k):
        dim = ORDERS[t][k]
        lines = math.prod(sizes[dim] for dim in ORDERS[t][k + 1:])
        piece = taken(t, k - 1)
        send, recv = hop_sends[3 * t + k], hop_recvs[3 * t + k]
        for j in range(1, sizes[dim]):
            part_of = piece[j * lines:(j + 1) * lines]
            if lines == 1:
                part_of = fold(part_of)
            send[j - 1] = part_of.astype(jnp.bfloat16)
            push(send.at[j - 1], recv.at[j - 1], send_sems.at[2], hop_sems.at[3 * t + k], peer_of[dim](j))
        mine[t][:lines] = piece[:lines]

    def first(t):
        hop(t, 0)

    def second(t):
        hop(t, 1)

    def third(t):
        hop(t, 2)

    reach = small_send.shape[2] // 2
    stages = [(1, lambda j: sibling)] + [(sizes[dim] - 1, peer_of[dim]) for dim in SMALL]

    def small_start():
        lane = lax.broadcasted_iota(jnp.int32, (rows, reach), 1).astype(jnp.float32)
        hits = jnp.where(lane == cls_col, 1.0, 0.0)
        small_send[0, :, :reach] = jnp.sum(hits, axis=0, keepdims=True)
        small_send[0, :, reach:] = jnp.sum(hits * sums["wedge"], axis=0, keepdims=True)
        small_push(0)

    def small_push(k):
        at = sum(n for n, _ in stages[:k])
        for j in range(stages[k][0]):
            push(small_send.at[k], small_recv.at[at + j], send_sems.at[3], small_sems.at[k], stages[k][1](j + 1))

    def small_take(k):
        at, n = sum(n for n, _ in stages[:k]), stages[k][0]
        tally = small_send[k]
        if n:
            arrived(small_recv.at[pl.ds(at, n)], small_sems.at[k])
        for j in range(n):
            tally = tally + small_recv[at + j]
        return tally

    def small_next(k):
        small_send[k + 1] = small_take(k)
        small_push(k + 1)

    nt = (((1,), (1,)), ((), ()))
    table = []

    def position(at):
        before = 0
        for begin, end in early + late:
            if begin <= at < end:
                return before + at - begin
            before += end - begin

    order = jnp.concatenate([ids[begin:end] for begin, end in early + late], axis=0)

    def prepare(runs):
        for begin, end in runs:
            lines = slice(begin, end)
            for t in range(CHUNKS):
                cols = slice(starts[t], starts[t] + widths[t])
                both = jnp.swapaxes(all_ref[lines, :, cols].astype(jnp.float32), 0, 1)
                real, imag = both[0], both[1]
                to = slice(position(begin), position(begin) + end - begin)
                ready[0, to, cols] = real.astype(jnp.bfloat16)
                ready[1, to, cols] = imag.astype(jnp.bfloat16)
                ready[2, to, cols] = (real * real + imag * imag).astype(jnp.bfloat16)

    def score(begin, end):
        power = sums["power"]
        for at in range(begin, end, 32):
            lines = slice(at, min(at + 32, end))
            group = lines.stop - lines.start
            inter = jnp.zeros((rows, group), jnp.float32)
            energy = jnp.zeros((rows, group), jnp.float32)
            for t in range(CHUNKS):
                width, span = widths[t], spans[t]
                cols = slice(starts[t], starts[t] + width)
                inter = inter + lax.dot_general(data[t][:, :width], ready[0, lines, cols], nt, preferred_element_type=jnp.float32)
                inter = inter + lax.dot_general(data[t][:, span:span + width], ready[1, lines, cols], nt, preferred_element_type=jnp.float32)
                energy = energy + lax.dot_general(low[:, cols], ready[2, lines, cols], nt, preferred_element_type=jnp.float32)
            value = inter / (math.sqrt(coef) * jnp.sqrt((energy / coef + EPS) * (power / coef + EPS)))
            lane = lax.broadcasted_iota(jnp.int32, (group, classes), 1)
            place = jnp.where(order[lines] == lane, 1.0, 0.0)
            table.append(jnp.dot(value, place, precision=lax.Precision.HIGHEST, preferred_element_type=jnp.float32))

    def score_early():
        prepare([(begin, end) for begin, end in early if end <= half])
        arrived(all_ref.at[pl.ds(0, half - diag)], ag_sems.at[0])
        prepare([(begin, end) for begin, end in early if end > half])

    def score_late():
        last = (gx - 1) * (gy - 1) * (gz - split(PIECES - 1)[0])
        if diag > last:
            arrived(all_ref.at[pl.ds(0, diag - last)], ag_sems.at[1])
        if last:
            arrived(all_ref.at[pl.ds(0, last), :, front], ag_sems.at[cross])
            arrived(all_ref.at[pl.ds(0, last), :, back], ag_sems.at[cross + 1])
        prepare(late)
        score(classes - 2 * diag, classes)
        scores_ref[...] = sum(table[1:], table[0])

    floors = []

    def counts():
        tally = small_take(3)
        load_ref[...] = tally[:, :classes] * classes / total
        lane = lax.broadcasted_iota(jnp.int32, (1, reach), 1)
        wedge_total = jnp.sum(jnp.where(lane == me, tally[:, reach:], 0.0), axis=1, keepdims=True)
        floors.append(TAU * (wedge_total / coef + 1.0))

    def means(t):
        whole = taken(t, 2)
        flat = jnp.concatenate([whole[0:1], whole[1:2]], axis=1)
        span, width, start = spans[t], widths[t], starts[t]
        scale = 1.0 / (flat[:, 2 * span:2 * span + width] + floors[0])
        for q in range(2):
            means_ref[0, q:q + 1, start:start + width] = flat[:, q * span:q * span + width] * scale

    compute(0)
    pl.semaphore_wait(barrier, len(peers))
    ag_own()
    cores(0)
    compute(1)
    cores(1)
    compute(2)
    cores(2)
    compute(3)
    cores(3)
    hop(0, 0)
    hop(1, 0)
    compute(4)
    cores(4)
    compute(5)
    cores(5)
    small_start()
    hop(2, 0)
    hop(3, 0)
    ag_forward(-1)
    small_next(0)
    hop(4, 0)
    hop(5, 0)
    hop(0, 1)
    hop(1, 1)
    ag_z()
    ag_direct(0)
    ag_direct(1)
    ag_direct(2)
    ag_core(-1)
    hop(2, 1)
    hop(3, 1)
    small_next(1)
    hop(4, 1)
    hop(5, 1)
    ag_forward(0)
    hop(0, 2)
    hop(1, 2)
    ag_forward(1)
    ag_forward(2)
    small_next(2)
    hop(2, 2)
    hop(3, 2)
    hop(4, 2)
    hop(5, 2)
    score_early()
    ag_core(0)
    ag_core(1)
    score(0, classes - 2 * diag)
    ag_core(2)
    score_late()
    counts()
    means(0)
    means(1)
    means(2)
    means(3)
    means(4)
    means(5)

    whole_of(all_ref.at[pl.ds(0, classes - 1)], send_sems.at[0]).wait_send()
    whole_of(ready.at[:, :half, :], send_sems.at[1]).wait_send()
    whole_of(all_ref.at[pl.ds(0, classes - 2), :, :3 * sum(spans) // 4], send_sems.at[2]).wait_send()
    whole_of(small_recv, send_sems.at[3]).wait_send()


def finish(*arrays):
    n = len(arrays)

    def put(*refs):
        sems = refs[2 * n]
        copies = [pltpu.make_async_copy(refs[i], refs[n + i], sems.at[i]) for i in range(n)]
        for copy in copies:
            copy.start()
        for copy in copies:
            copy.wait()

    scores, means, load = pl.pallas_call(
        put,
        out_shape=tuple(jax.ShapeDtypeStruct(a.shape, a.dtype) for a in arrays),
        in_specs=[pl.BlockSpec(memory_space=pltpu.VMEM)] * n,
        out_specs=(pl.BlockSpec(memory_space=pltpu.HBM),) * n,
        scratch_shapes=[pltpu.SemaphoreType.DMA((n,))],
        compiler_params=pltpu.CompilerParams(vmem_limit_bytes=1024 * 1024),
    )(*arrays)
    return (scores, means, load[0])


def body(particles, references, assignment, orientation, tilt_range):
    part_rows = particles.shape[0]
    coef = particles.shape[2]
    devices = lax.axis_size("dom")
    classes = references.shape[0] * devices
    assert references.shape[0] == 1
    gx, gy, gz = factor(devices)
    total = part_rows * devices
    spans = spans_of(coef)
    padded = sum(spans)
    width = 2 * (-(-classes // LANES) * LANES)
    half = classes // 2

    vmem = pl.BlockSpec(memory_space=pltpu.VMEM)
    hbm = pl.BlockSpec(memory_space=pltpu.HBM)
    dma = pltpu.SemaphoreType.DMA
    bf16, f32, i32 = jnp.bfloat16, jnp.float32, jnp.int32

    sizes = {"x": gx, "y": gy, "z": gz}
    hops = []
    for order, span in zip(ORDERS, spans):
        wide = 3 * span
        for k, dim in enumerate(order):
            lines = math.prod(sizes[d] for d in order[k + 1:])
            shape = (lines, wide) if lines > 1 else (2, wide // 2)
            hops.append(((max(1, sizes[dim] - 1), *shape), bf16))
    buffers = [
        ((part_rows, 2, coef), bf16),
        ((1, part_rows), i32),
        ((1, part_rows), i32),
        ((2, part_rows), i32),
        ((part_rows, padded), bf16),
        ((classes, 2, coef), bf16),
        ((3, classes, padded), bf16),
        ((4, 1, width), f32),
        ((gx + gy + gz - 2, 1, width), f32),
        *hops, *hops,
        *[((part_rows, 3 * span), bf16) for span in spans],
        *[((half, 3 * span), f32) for span in spans],
        *[((half, 3 * span), bf16) for span in spans],
        *[((half, 3 * span), bf16) for span in spans],
    ]
    held = sum(math.prod(shape) * jnp.dtype(kind).itemsize for shape, kind in buffers)
    limit = min(60, held // 2**20 + 8) * 2**20
    scores, means, load = pl.pallas_call(
        functools.partial(kernel, gx, gy, gz, spans, coef, total),
        out_shape=(
            jax.ShapeDtypeStruct((part_rows, classes), f32),
            jax.ShapeDtypeStruct((1, 2, coef), f32),
            jax.ShapeDtypeStruct((1, classes), f32),
        ),
        in_specs=[hbm] * 5,
        out_specs=(vmem, vmem, vmem),
        scratch_shapes=[pltpu.VMEM(shape, kind) for shape, kind in buffers] + [
            dma((4 + CHUNKS,)), dma((3 + 4 * (PIECES + 1) + 2,)), dma((CHUNKS,)), dma((3 * CHUNKS,)), dma((4,)), dma((4,)),
        ],
        compiler_params=pltpu.CompilerParams(
            collective_id=0, has_side_effects=True, vmem_limit_bytes=limit
        ),
    )(*[
        pltpu.with_memory_space_constraint(v, pltpu.HBM)
        for v in (particles, references, assignment.reshape(1, part_rows), orientation[None, :], tilt_range)
    ])
    return finish(scores, means, load)


def solution(mesh):
    in_specs = (
        P("dom", None, None),
        P("dom", None, None),
        P("dom", None),
        P("dom"),
        P(None, "dom"),
    )
    out_specs = (P("dom", None), P("dom", None, None), P())
    return jax.shard_map(body, mesh=mesh, in_specs=in_specs, out_specs=out_specs, check_vma=False)
```

```python
import functools
import math

import jax
import jax.numpy as jnp
from jax import lax
from jax.experimental import pallas as pl
from jax.experimental.pallas import tpu as pltpu
from jax.sharding import PartitionSpec as P

GRID = 24
ORIENTS = 36
EPS = 1e-06
GAIN = 6.0
TAU = 0.5
LANES = 128
MESH = pl.DeviceIdType.MESH

SHARES = (14, 14, 8, 8, 8, 8)
CHUNKS = len(SHARES)
SUB = 640
ORDERS = ("xzy", "yzx", "xyz", "yxz", "xyz", "yxz")
SMALL = "xyz"
PIECES = 3


def factor(devices):
    chips = devices // 2
    log = chips.bit_length() - 1
    gx = 1 << (log // 3)
    gy = 1 << ((log - log // 3) // 2)
    return gx, gy, chips // (gx * gy)


def spans_of(coef):
    unit = sum(SHARES)
    pairs = -(-coef // (4 * LANES)) * 2
    ends = [sum(SHARES[:t + 1]) * pairs // unit for t in range(CHUNKS)]
    return [(end - start) * 2 * LANES for start, end in zip([0] + ends, ends)]


def column(row):
    rows = row.shape[1]
    line = lax.broadcasted_iota(jnp.int32, (rows, rows), 0)
    lane = lax.broadcasted_iota(jnp.int32, (rows, rows), 1)
    return jnp.sum(jnp.where(line == lane, row, 0.0), axis=1, keepdims=True)


def frequencies(first, width):
    index = (lax.broadcasted_iota(jnp.int32, (1, width), 1) + first).astype(jnp.float32)
    plane = jnp.floor((index + 0.5) * (1.0 / (GRID * GRID)))
    rest = index - plane * (GRID * GRID)
    col_x = jnp.floor((rest + 0.5) * (1.0 / GRID))
    col_z = rest - col_x * GRID
    freq_x = jnp.where(col_x >= GRID // 2, col_x - GRID, col_x)
    freq_z = jnp.where(col_z >= GRID // 2, col_z - GRID, col_z)
    return freq_x, plane, freq_z, index


def kernel(
    gx, gy, gz, spans, coef, total,
    part_hbm, ref_hbm, cls_hbm, orient_hbm, tilt_hbm,
    scores_ref, means_ref, load_ref,
    part, cls_ref, orient_ref, tilt_ref,
    low, all_ref, ready, small_send, small_recv, *rest,
):
    hop_sends, hop_recvs = rest[:3 * CHUNKS], rest[3 * CHUNKS:6 * CHUNKS]
    data, mine, send_core, recv_core = (rest[k * CHUNKS:(k + 1) * CHUNKS] for k in range(6, 10))
    in_sems, ag_sems, core_sems, hop_sems, small_sems, send_sems = rest[10 * CHUNKS:]
    starts = [sum(spans[:t]) for t in range(CHUNKS)]
    widths = [max(0, min(spans[t], coef - starts[t])) for t in range(CHUNKS)]
    me = lax.axis_index("dom")
    core = lax.rem(me, 2)
    chip = me // 2
    x = lax.rem(chip, gx)
    y = lax.rem(chip // gx, gy)
    z = chip // (gx * gy)
    sibling = me + 1 - 2 * core
    classes = 2 * gx * gy * gz
    half = classes // 2
    rows = part.shape[0]
    cut = coef // 2 // LANES * LANES

    def device(x_at, y_at, z_at, c_at):
        return ((z_at * gy + y_at) * gx + x_at) * 2 + c_at

    def x_peer(j):
        return device(lax.rem(x + j, gx), y, z, core)

    def y_peer(j):
        return device(x, lax.rem(y + j, gy), z, core)

    def x_cross(j):
        return device(lax.rem(x + j, gx), y, z, 1 - core)

    def y_cross(j):
        return device(x, lax.rem(y + j, gy), z, 1 - core)

    def z_cross(j):
        return device(x, y, lax.rem(z + j, gz), 1 - core)

    def z_peer(j):
        return device(x, y, lax.rem(z + j, gz), core)

    sizes = {"x": gx, "y": gy, "z": gz}
    peer_of = {"x": x_peer, "y": y_peer, "z": z_peer}
    cross_of = {"x": x_cross, "y": y_cross, "z": z_cross}

    def fetch(src, dst, at):
        copy = pltpu.make_async_copy(src, dst, in_sems.at[at])
        copy.start()
        return copy

    barrier = pltpu.get_barrier_semaphore()
    peers = [sibling]
    peers += [x_peer(j) for j in range(1, gx)]
    peers += [y_peer(j) for j in range(1, gy)]
    peers += [z_peer(j) for j in range(1, gz)]
    peers += [x_cross(j) for j in range(1, gx)]
    peers += [y_cross(j) for j in range(1, gy)]
    peers += [z_cross(j) for j in range(1, gz)]
    for peer in peers:
        pl.semaphore_signal(barrier, inc=1, device_id=(peer,), device_id_type=MESH)
    metas = [
        fetch(orient_hbm, orient_ref, 1),
        fetch(tilt_hbm, tilt_ref, 2),
        fetch(cls_hbm, cls_ref, 3),
    ]
    own_ref = fetch(ref_hbm.at[0], all_ref.at[0], 0)
    part_copies = []
    for t in range(CHUNKS):
        cols = pl.ds(starts[t], widths[t])
        part_copies.append(fetch(part_hbm.at[:, :, cols], part.at[:, :, cols], 4 + t))

    def push(src, dst, send_sem, recv_sem, target):
        pltpu.make_async_remote_copy(
            src_ref=src, dst_ref=dst, send_sem=send_sem, recv_sem=recv_sem,
            device_id=(target,), device_id_type=MESH,
        ).start()

    def whole_of(ref, sem):
        return pltpu.make_async_remote_copy(
            src_ref=ref, dst_ref=ref, send_sem=sem, recv_sem=sem,
            device_id=(sibling,), device_id_type=MESH,
        )

    def arrived(ref, sem):
        whole_of(ref, sem).wait_recv()

    def slot(dx, dy, dc):
        return ((dc * gx + dx) * gy + dy) * gz

    def give(src_slot, dst_slot, n, lanes, at, target):
        src = all_ref.at[pl.ds(src_slot, n), :, lanes]
        dst = all_ref.at[pl.ds(dst_slot, n), :, lanes]
        push(src, dst, send_sems.at[0], ag_sems.at[at], target)

    every = slice(0, coef)
    front, back = slice(0, cut), slice(cut, coef)

    def split(g):
        return 1 + g * (gz - 1) // PIECES, 1 + (g + 1) * (gz - 1) // PIECES

    def sem_of(g):
        return 3 + 4 * (g + 1)

    cross = sem_of(PIECES)

    def ag_direct(g):
        at, end = split(g) if g >= 0 else (0, 1)
        sem = sem_of(g)
        if at == end:
            return
        for j in range(1, gx):
            give(at, slot(gx - j, 0, 1) + at, end - at, every, sem, x_cross(j))
        for j in range(1, gy):
            give(at, slot(0, gy - j, 1) + at, end - at, every, sem + 1, y_cross(j))
        give(at, slot(0, 0, 1) + at, end - at, every, 0, sibling)

    def ag_forward(g):
        at, end = split(g) if g >= 0 else (0, 1)
        n, sem = end - at, sem_of(g)
        if n == 0:
            return
        if gx > 1:
            arrived(all_ref.at[pl.ds(0, (gx - 1) * n)], ag_sems.at[sem])
        for dx in range(1, gx):
            for j in range(1, gy):
                give(slot(dx, 0, 1) + at, slot(dx, gy - j, 1) + at, n, front, sem + 2, y_peer(j))
                if g == PIECES - 1:
                    give(slot(dx, 0, 1) + at, slot(dx, gy - j, 0) + at, n, front, cross, y_cross(j))
        if gy > 1:
            arrived(all_ref.at[pl.ds(0, (gy - 1) * n)], ag_sems.at[sem + 1])
        for dy in range(1, gy):
            for j in range(1, gx):
                give(slot(0, dy, 1) + at, slot(gx - j, dy, 1) + at, n, back, sem + 3, x_peer(j))
                if g == PIECES - 1:
                    give(slot(0, dy, 1) + at, slot(gx - j, dy, 0) + at, n, back, cross + 1, x_cross(j))
        for dx in range(1, gx):
            give(slot(dx, 0, 1) + at, slot(dx, 0, 0) + at, n, every, 0, sibling)
        for dy in range(1, gy):
            give(slot(0, dy, 1) + at, slot(0, dy, 0) + at, n, every, 0, sibling)

    def ag_core(g):
        at, end = split(g) if g >= 0 else (0, 1)
        n, sem = end - at, sem_of(g)
        count = (gx - 1) * (gy - 1) * n
        if count:
            arrived(all_ref.at[pl.ds(0, count), :, front], ag_sems.at[sem + 2])
            arrived(all_ref.at[pl.ds(0, count), :, back], ag_sems.at[sem + 3])
        if g == PIECES - 1:
            return
        for dx in range(1, gx):
            for dy in range(1, gy):
                give(slot(dx, dy, 1) + at, slot(dx, dy, 0) + at, n, every, 1, sibling)

    def ag_own():
        own_ref.wait()
        for j in range(1, gz):
            give(0, gz - j, 1, every, 2, z_peer(j))
        ag_direct(-1)

    def ag_z():
        if gz > 1:
            arrived(all_ref.at[pl.ds(1, gz - 1)], ag_sems.at[2])

    diag = (gx - 1) * (gy - 1) * gz
    early, late = [], []
    for dc in range(2):
        for dx in range(gx):
            for dy in range(gy):
                runs = late if dx and dy else early
                at = slot(dx, dy, dc)
                if runs and runs[-1][1] == at and at != half:
                    runs[-1] = (runs[-1][0], at + gz)
                else:
                    runs.append((at, at + gz))

    for copy in metas:
        copy.wait()
    angle = orient_ref[...].astype(jnp.float32) * (2.0 * math.pi / ORIENTS)
    bins = tilt_ref[...].astype(jnp.float32)
    low_end = -(40.0 + 1.5 * bins[0:1]) * (math.pi / 180.0)
    high_end = (40.0 + 1.5 * bins[1:2]) * (math.pi / 180.0)
    sin_a, cos_a = column(jnp.sin(angle)), column(jnp.cos(angle))
    cos_c = column(jnp.cos(low_end + high_end))
    sin_c = column(jnp.sin(low_end + high_end))
    cos_w = column(jnp.cos(high_end - low_end))
    cls_row = cls_ref[...].astype(jnp.float32)
    cls_col = column(cls_row)

    def log2(n):
        return n.bit_length() - 1

    row = lax.broadcasted_iota(jnp.int32, (classes, 1), 0)

    def ids_of(order, flip):
        left, at = row, {}
        for dim in reversed(order):
            at[dim] = left & (sizes[dim] - 1)
            left = lax.shift_right_logical(left, log2(sizes[dim]))
        return device((at["x"] + x) & (gx - 1), (at["y"] + y) & (gy - 1), (at["z"] + z) & (gz - 1), (left + core + flip) & 1)

    ids = ids_of("xyz", 0)
    onehot = {}
    for order in ORDERS:
        if order not in onehot:
            onehot[order] = jnp.where(ids_of(order, 1).astype(jnp.float32) == cls_row, 1.0, 0.0).astype(jnp.bfloat16)
    sums = {"wedge": jnp.zeros((rows, 1), jnp.float32), "power": jnp.zeros((rows, 1), jnp.float32)}

    def parts(first, size):
        width = max(0, min(size, coef - first))
        pieces = []
        if width:
            both = part[:, :, first:first + width].astype(jnp.float32)
            pieces.append(jnp.swapaxes(both, 0, 1))
        if width < size:
            pieces.append(jnp.zeros((2, rows, size - width), jnp.float32))
        both = jnp.concatenate(pieces, axis=2) if len(pieces) > 1 else pieces[0]
        return both[0], both[1]

    def wedges(first, size):
        freq_x, freq_y, freq_z, index = frequencies(first, size)
        along = freq_y * cos_a - freq_x * sin_a
        along_sq = along * along
        z_sq = freq_z * freq_z
        scale = 1.0 / (along_sq + (z_sq + 1.0))
        value = ((along_sq - z_sq) * cos_c - (2.0 * along * freq_z) * sin_c) * scale - cos_w
        wedge = 1.0 / (1.0 + jnp.exp(value * (-GAIN)))
        inside = wedge if first + size <= coef else jnp.where(index < coef, wedge, 0.0)
        sums["wedge"] = sums["wedge"] + jnp.sum(inside, axis=1, keepdims=True)
        return wedge

    def compute(t):
        span = spans[t]
        part_copies[t].wait()
        for at in range(0, span, SUB):
            first = starts[t] + at
            size = min(SUB, span - at)
            wedge = wedges(first, size)
            real, imag = parts(first, size)
            sums["power"] = sums["power"] + jnp.sum(wedge * (real * real + imag * imag), axis=1, keepdims=True)
            data[t][:, at:at + size] = (wedge * real).astype(jnp.bfloat16)
            data[t][:, span + at:span + at + size] = (wedge * imag).astype(jnp.bfloat16)
            data[t][:, 2 * span + at:2 * span + at + size] = (wedge * wedge).astype(jnp.bfloat16)
            low[:, first:first + size] = wedge.astype(jnp.bfloat16)
        for q in range(3):
            cols = slice(q * span, (q + 1) * span)
            both = jnp.dot(onehot[ORDERS[t]], data[t][:, cols], preferred_element_type=jnp.float32)
            send_core[t][:, cols] = both[half:].astype(jnp.bfloat16)
            mine[t][:, cols] = both[:half]

    def cores(t):
        push(send_core[t], recv_core[t], send_sems.at[1], core_sems.at[t], sibling)

    def fold(line):
        wide = line.shape[1]
        return jnp.concatenate([line[:, :wide // 2], line[:, wide // 2:]], axis=0)

    def taken(t, k):
        if k < 0:
            arrived(recv_core[t], core_sems.at[t])
            return mine[t][...] + recv_core[t][...].astype(jnp.float32)
        n = sizes[ORDERS[t][k]]
        lines = math.prod(sizes[dim] for dim in ORDERS[t][k + 1:])
        recv = hop_recvs[3 * t + k]
        if k == 1 or n > 1:
            arrived(recv, hop_sems.at[3 * t + k])
        if k == 1:
            piece = recv[0].astype(jnp.float32)
            for j in range(1, n):
                piece = piece + recv[j].astype(jnp.float32)
            return piece
        piece = mine[t][:lines]
        if lines == 1:
            piece = fold(piece)
        for j in range(1, n):
            piece = piece + recv[j - 1].astype(jnp.float32)
        return piece

    def hop(t, k):
        dim = ORDERS[t][k]
        lines = math.prod(sizes[dim] for dim in ORDERS[t][k + 1:])
        piece = taken(t, k - 1)
        send, recv = hop_sends[3 * t + k], hop_recvs[3 * t + k]
        for j in range(0 if k == 1 else 1, sizes[dim]):
            part_of = piece[j * lines:(j + 1) * lines]
            if lines == 1:
                part_of = fold(part_of)
            at = j if k == 1 else j - 1
            send[at] = part_of.astype(jnp.bfloat16)
            peer = sibling if j == 0 else (cross_of if k == 1 else peer_of)[dim](j)
            sem = 4 + t if j == 0 else 2
            push(send.at[at], recv.at[at], send_sems.at[sem], hop_sems.at[3 * t + k], peer)
        if k != 1:
            mine[t][:lines] = piece[:lines]

    def first(t):
        hop(t, 0)

    def second(t):
        hop(t, 1)

    def third(t):
        hop(t, 2)

    reach = small_send.shape[2] // 2
    stages = [(1, lambda j: sibling)] + [(sizes[dim] - 1, (peer_of, cross_of, peer_of)[k][dim]) for k, dim in enumerate(SMALL)]

    def small_start():
        lane = lax.broadcasted_iota(jnp.int32, (rows, reach), 1).astype(jnp.float32)
        hits = jnp.where(lane == cls_col, 1.0, 0.0)
        small_send[0, :, :reach] = jnp.sum(hits, axis=0, keepdims=True)
        small_send[0, :, reach:] = jnp.sum(hits * sums["wedge"], axis=0, keepdims=True)
        small_push(0)

    def small_push(k):
        at = sum(n for n, _ in stages[:k])
        for j in range(stages[k][0]):
            push(small_send.at[k], small_recv.at[at + j], send_sems.at[3], small_sems.at[k], stages[k][1](j + 1))

    def small_take(k):
        at, n = sum(n for n, _ in stages[:k]), stages[k][0]
        tally = small_send[k]
        if n:
            arrived(small_recv.at[pl.ds(at, n)], small_sems.at[k])
        for j in range(n):
            tally = tally + small_recv[at + j]
        return tally

    def small_next(k):
        small_send[k + 1] = small_take(k)
        small_push(k + 1)

    nt = (((1,), (1,)), ((), ()))
    table = []

    def position(at):
        before = 0
        for begin, end in early + late:
            if begin <= at < end:
                return before + at - begin
            before += end - begin

    order = jnp.concatenate([ids[begin:end] for begin, end in early + late], axis=0)

    def prepare(runs):
        for begin, end in runs:
            lines = slice(begin, end)
            for t in range(CHUNKS):
                cols = slice(starts[t], starts[t] + widths[t])
                both = jnp.swapaxes(all_ref[lines, :, cols].astype(jnp.float32), 0, 1)
                real, imag = both[0], both[1]
                to = slice(position(begin), position(begin) + end - begin)
                ready[0, to, cols] = real.astype(jnp.bfloat16)
                ready[1, to, cols] = imag.astype(jnp.bfloat16)
                ready[2, to, cols] = (real * real + imag * imag).astype(jnp.bfloat16)

    def score(begin, end):
        power = sums["power"]
        for at in range(begin, end, 32):
            lines = slice(at, min(at + 32, end))
            group = lines.stop - lines.start
            inter = jnp.zeros((rows, group), jnp.float32)
            energy = jnp.zeros((rows, group), jnp.float32)
            for t in range(CHUNKS):
                width, span = widths[t], spans[t]
                cols = slice(starts[t], starts[t] + width)
                inter = inter + lax.dot_general(data[t][:, :width], ready[0, lines, cols], nt, preferred_element_type=jnp.float32)
                inter = inter + lax.dot_general(data[t][:, span:span + width], ready[1, lines, cols], nt, preferred_element_type=jnp.float32)
                energy = energy + lax.dot_general(low[:, cols], ready[2, lines, cols], nt, preferred_element_type=jnp.float32)
            value = inter / (math.sqrt(coef) * jnp.sqrt((energy / coef + EPS) * (power / coef + EPS)))
            lane = lax.broadcasted_iota(jnp.int32, (group, classes), 1)
            place = jnp.where(order[lines] == lane, 1.0, 0.0)
            table.append(jnp.dot(value, place, precision=lax.Precision.HIGHEST, preferred_element_type=jnp.float32))

    groups = [(at, at + gz) for begin, end in early for at in range(begin, end, gz)]

    def merged(runs):
        out = []
        for begin, end in runs:
            if out and out[-1][1] == begin and begin != half:
                out[-1] = (out[-1][0], end)
            else:
                out.append((begin, end))
        return out

    def prepare_near():
        prepare(merged([g for g in groups if (g[0] < half) == (g[0] % half == 0)]))

    def prepare_far():
        arrived(all_ref.at[pl.ds(0, half - diag)], ag_sems.at[0])
        prepare(merged([g for g in groups if (g[0] < half) != (g[0] % half == 0)]))

    def score_late():
        last = (gx - 1) * (gy - 1) * (gz - split(PIECES - 1)[0])
        if diag > last:
            arrived(all_ref.at[pl.ds(0, diag - last)], ag_sems.at[1])
        if last:
            arrived(all_ref.at[pl.ds(0, last), :, front], ag_sems.at[cross])
            arrived(all_ref.at[pl.ds(0, last), :, back], ag_sems.at[cross + 1])
        prepare(late)
        score(classes - 2 * diag, classes)
        scores_ref[...] = sum(table[1:], table[0])

    floors = []

    def counts():
        tally = small_take(3)
        load_ref[...] = tally[:, :classes] * classes / total
        lane = lax.broadcasted_iota(jnp.int32, (1, reach), 1)
        wedge_total = jnp.sum(jnp.where(lane == me, tally[:, reach:], 0.0), axis=1, keepdims=True)
        floors.append(TAU * (wedge_total / coef + 1.0))

    def means(t):
        whole = taken(t, 2)
        flat = jnp.concatenate([whole[0:1], whole[1:2]], axis=1)
        span, width, start = spans[t], widths[t], starts[t]
        scale = 1.0 / (flat[:, 2 * span:2 * span + width] + floors[0])
        for q in range(2):
            means_ref[0, q:q + 1, start:start + width] = flat[:, q * span:q * span + width] * scale

    compute(0)
    pl.semaphore_wait(barrier, len(peers))
    ag_own()
    cores(0)
    compute(1)
    cores(1)
    compute(2)
    cores(2)
    compute(3)
    cores(3)
    hop(0, 0)
    hop(1, 0)
    compute(4)
    cores(4)
    compute(5)
    cores(5)
    small_start()
    hop(2, 0)
    hop(3, 0)
    ag_forward(-1)
    small_next(0)
    hop(4, 0)
    hop(5, 0)
    hop(0, 1)
    hop(1, 1)
    ag_z()
    ag_direct(0)
    ag_direct(1)
    ag_direct(2)
    hop(2, 1)
    hop(3, 1)
    ag_core(-1)
    small_next(1)
    hop(4, 1)
    hop(5, 1)
    ag_forward(0)
    ag_forward(1)
    ag_forward(2)
    small_next(2)
    hop(2, 2)
    hop(3, 2)
    hop(4, 2)
    hop(5, 2)
    hop(0, 2)
    hop(1, 2)
    prepare_near()
    ag_core(0)
    ag_core(1)
    prepare_far()
    score(0, classes - 2 * diag)
    ag_core(2)
    score_late()
    counts()
    means(0)
    means(1)
    means(2)
    means(3)
    means(4)
    means(5)

    whole_of(all_ref.at[pl.ds(0, classes - 1)], send_sems.at[0]).wait_send()
    whole_of(ready.at[:, :half, :], send_sems.at[1]).wait_send()
    whole_of(all_ref.at[pl.ds(0, classes - 2), :, :3 * sum(spans) // 4], send_sems.at[2]).wait_send()
    whole_of(small_recv, send_sems.at[3]).wait_send()
    for t in range(CHUNKS):
        whole_of(hop_sends[3 * t + 1].at[0], send_sems.at[4 + t]).wait_send()


def finish(*arrays):
    n = len(arrays)

    def put(*refs):
        sems = refs[2 * n]
        copies = [pltpu.make_async_copy(refs[i], refs[n + i], sems.at[i]) for i in range(n)]
        for copy in copies:
            copy.start()
        for copy in copies:
            copy.wait()

    scores, means, load = pl.pallas_call(
        put,
        out_shape=tuple(jax.ShapeDtypeStruct(a.shape, a.dtype) for a in arrays),
        in_specs=[pl.BlockSpec(memory_space=pltpu.VMEM)] * n,
        out_specs=(pl.BlockSpec(memory_space=pltpu.HBM),) * n,
        scratch_shapes=[pltpu.SemaphoreType.DMA((n,))],
        compiler_params=pltpu.CompilerParams(vmem_limit_bytes=1024 * 1024),
    )(*arrays)
    return (scores, means, load[0])


def body(particles, references, assignment, orientation, tilt_range):
    part_rows = particles.shape[0]
    coef = particles.shape[2]
    devices = lax.axis_size("dom")
    classes = references.shape[0] * devices
    assert references.shape[0] == 1
    gx, gy, gz = factor(devices)
    total = part_rows * devices
    spans = spans_of(coef)
    padded = sum(spans)
    width = 2 * (-(-classes // LANES) * LANES)
    half = classes // 2

    vmem = pl.BlockSpec(memory_space=pltpu.VMEM)
    hbm = pl.BlockSpec(memory_space=pltpu.HBM)
    dma = pltpu.SemaphoreType.DMA
    bf16, f32, i32 = jnp.bfloat16, jnp.float32, jnp.int32

    sizes = {"x": gx, "y": gy, "z": gz}
    hops = []
    for order, span in zip(ORDERS, spans):
        wide = 3 * span
        for k, dim in enumerate(order):
            lines = math.prod(sizes[d] for d in order[k + 1:])
            shape = (lines, wide) if lines > 1 else (2, wide // 2)
            hops.append(((max(1, sizes[dim] - (k != 1)), *shape), bf16))
    buffers = [
        ((part_rows, 2, coef), bf16),
        ((1, part_rows), i32),
        ((1, part_rows), i32),
        ((2, part_rows), i32),
        ((part_rows, padded), bf16),
        ((classes, 2, coef), bf16),
        ((3, classes, padded), bf16),
        ((4, 1, width), f32),
        ((gx + gy + gz - 2, 1, width), f32),
        *hops, *hops,
        *[((part_rows, 3 * span), bf16) for span in spans],
        *[((half, 3 * span), f32) for span in spans],
        *[((half, 3 * span), bf16) for span in spans],
        *[((half, 3 * span), bf16) for span in spans],
    ]
    held = sum(math.prod(shape) * jnp.dtype(kind).itemsize for shape, kind in buffers)
    limit = min(60, held // 2**20 + 8) * 2**20
    scores, means, load = pl.pallas_call(
        functools.partial(kernel, gx, gy, gz, spans, coef, total),
        out_shape=(
            jax.ShapeDtypeStruct((part_rows, classes), f32),
            jax.ShapeDtypeStruct((1, 2, coef), f32),
            jax.ShapeDtypeStruct((1, classes), f32),
        ),
        in_specs=[hbm] * 5,
        out_specs=(vmem, vmem, vmem),
        scratch_shapes=[pltpu.VMEM(shape, kind) for shape, kind in buffers] + [
            dma((4 + CHUNKS,)), dma((3 + 4 * (PIECES + 1) + 2,)), dma((CHUNKS,)), dma((3 * CHUNKS,)), dma((4,)), dma((4 + CHUNKS,)),
        ],
        compiler_params=pltpu.CompilerParams(
            collective_id=0, has_side_effects=True, vmem_limit_bytes=limit
        ),
    )(*[
        pltpu.with_memory_space_constraint(v, pltpu.HBM)
        for v in (particles, references, assignment.reshape(1, part_rows), orientation[None, :], tilt_range)
    ])
    return finish(scores, means, load)


def solution(mesh):
    in_specs = (
        P("dom", None, None),
        P("dom", None, None),
        P("dom", None),
        P("dom"),
        P(None, "dom"),
    )
    out_specs = (P("dom", None), P("dom", None, None), P())
    return jax.shard_map(body, mesh=mesh, in_specs=in_specs, out_specs=out_specs, check_vma=False)
```

```python
import functools
import math

import jax
import jax.numpy as jnp
from jax import lax
from jax.experimental import pallas as pl
from jax.experimental.pallas import tpu as pltpu
from jax.sharding import PartitionSpec as P

GRID = 24
ORIENTS = 36
EPS = 1e-06
GAIN = 6.0
TAU = 0.5
LANES = 128
MESH = pl.DeviceIdType.MESH

SHARES = (14, 14, 8, 8, 8, 8)
CHUNKS = len(SHARES)
SUB = 640
ORDERS = ("xzy", "yzx", "xyz", "yxz", "xyz", "yxz")
SMALL = "xyz"
PIECES = 3


def factor(devices):
    chips = devices // 2
    log = chips.bit_length() - 1
    gx = 1 << (log // 3)
    gy = 1 << ((log - log // 3) // 2)
    return gx, gy, chips // (gx * gy)


def spans_of(coef):
    unit = sum(SHARES)
    pairs = -(-coef // (4 * LANES)) * 2
    ends = [sum(SHARES[:t + 1]) * pairs // unit for t in range(CHUNKS)]
    return [(end - start) * 2 * LANES for start, end in zip([0] + ends, ends)]


def column(row):
    rows = row.shape[1]
    line = lax.broadcasted_iota(jnp.int32, (rows, rows), 0)
    lane = lax.broadcasted_iota(jnp.int32, (rows, rows), 1)
    return jnp.sum(jnp.where(line == lane, row, 0.0), axis=1, keepdims=True)


def frequencies(first, width):
    index = (lax.broadcasted_iota(jnp.int32, (1, width), 1) + first).astype(jnp.float32)
    plane = jnp.floor((index + 0.5) * (1.0 / (GRID * GRID)))
    rest = index - plane * (GRID * GRID)
    col_x = jnp.floor((rest + 0.5) * (1.0 / GRID))
    col_z = rest - col_x * GRID
    freq_x = jnp.where(col_x >= GRID // 2, col_x - GRID, col_x)
    freq_z = jnp.where(col_z >= GRID // 2, col_z - GRID, col_z)
    return freq_x, plane, freq_z, index


def kernel(
    gx, gy, gz, spans, coef, total,
    part_hbm, ref_hbm, cls_hbm, orient_hbm, tilt_hbm,
    scores_ref, means_ref, load_ref,
    part, cls_ref, orient_ref, tilt_ref,
    low, all_ref, ready, small_send, small_recv, *rest,
):
    hop_sends, hop_recvs = rest[:3 * CHUNKS], rest[3 * CHUNKS:6 * CHUNKS]
    data, mine, send_core, recv_core = (rest[k * CHUNKS:(k + 1) * CHUNKS] for k in range(6, 10))
    extra = CHUNKS // 2
    core_pairs = recv_core[:CHUNKS // 2]
    recv_core = [core_pairs[t // 2].at[t % 2] for t in range(CHUNKS)]
    in_sems, ag_sems, core_sems, hop_sems, small_sems, send_sems = rest[10 * CHUNKS - extra:]
    starts = [sum(spans[:t]) for t in range(CHUNKS)]
    widths = [max(0, min(spans[t], coef - starts[t])) for t in range(CHUNKS)]
    me = lax.axis_index("dom")
    core = lax.rem(me, 2)
    chip = me // 2
    x = lax.rem(chip, gx)
    y = lax.rem(chip // gx, gy)
    z = chip // (gx * gy)
    sibling = me + 1 - 2 * core
    classes = 2 * gx * gy * gz
    half = classes // 2
    rows = part.shape[0]
    cut = coef // 2 // LANES * LANES

    def device(x_at, y_at, z_at, c_at):
        return ((z_at * gy + y_at) * gx + x_at) * 2 + c_at

    def x_peer(j):
        return device(lax.rem(x + j, gx), y, z, core)

    def y_peer(j):
        return device(x, lax.rem(y + j, gy), z, core)

    def x_cross(j):
        return device(lax.rem(x + j, gx), y, z, 1 - core)

    def y_cross(j):
        return device(x, lax.rem(y + j, gy), z, 1 - core)

    def z_cross(j):
        return device(x, y, lax.rem(z + j, gz), 1 - core)

    def z_peer(j):
        return device(x, y, lax.rem(z + j, gz), core)

    sizes = {"x": gx, "y": gy, "z": gz}
    peer_of = {"x": x_peer, "y": y_peer, "z": z_peer}
    cross_of = {"x": x_cross, "y": y_cross, "z": z_cross}

    def fetch(src, dst, at):
        copy = pltpu.make_async_copy(src, dst, in_sems.at[at])
        copy.start()
        return copy

    barrier = pltpu.get_barrier_semaphore()
    peers = [sibling]
    peers += [x_peer(j) for j in range(1, gx)]
    peers += [y_peer(j) for j in range(1, gy)]
    peers += [z_peer(j) for j in range(1, gz)]
    peers += [x_cross(j) for j in range(1, gx)]
    peers += [y_cross(j) for j in range(1, gy)]
    peers += [z_cross(j) for j in range(1, gz)]
    for peer in peers:
        pl.semaphore_signal(barrier, inc=1, device_id=(peer,), device_id_type=MESH)
    metas = [
        fetch(orient_hbm, orient_ref, 1),
        fetch(tilt_hbm, tilt_ref, 2),
        fetch(cls_hbm, cls_ref, 3),
    ]
    own_ref = fetch(ref_hbm.at[0], all_ref.at[0], 0)
    part_copies = []
    for t in range(0, CHUNKS, 2):
        cols = pl.ds(starts[t], widths[t] + widths[t + 1])
        part_copies.append(fetch(part_hbm.at[:, :, cols], part.at[:, :, cols], 4 + t // 2))

    def push(src, dst, send_sem, recv_sem, target):
        pltpu.make_async_remote_copy(
            src_ref=src, dst_ref=dst, send_sem=send_sem, recv_sem=recv_sem,
            device_id=(target,), device_id_type=MESH,
        ).start()

    def whole_of(ref, sem):
        return pltpu.make_async_remote_copy(
            src_ref=ref, dst_ref=ref, send_sem=sem, recv_sem=sem,
            device_id=(sibling,), device_id_type=MESH,
        )

    def arrived(ref, sem):
        whole_of(ref, sem).wait_recv()

    def slot(dx, dy, dc):
        return ((dc * gx + dx) * gy + dy) * gz

    def give(src_slot, dst_slot, n, lanes, at, target):
        src = all_ref.at[pl.ds(src_slot, n), :, lanes]
        dst = all_ref.at[pl.ds(dst_slot, n), :, lanes]
        push(src, dst, send_sems.at[0], ag_sems.at[at], target)

    every = slice(0, coef)
    front, back = slice(0, cut), slice(cut, coef)

    def split(g):
        return 1 + g * (gz - 1) // PIECES, 1 + (g + 1) * (gz - 1) // PIECES

    def sem_of(g):
        return 3 + 2 * (g + 1)

    cross = sem_of(PIECES)

    def ag_direct(g):
        at, end = split(g) if g >= 0 else (0, 1)
        sem = sem_of(g)
        if at == end:
            return
        for j in range(1, gx):
            give(at, slot(gx - j, 0, 1) + at, end - at, every, sem, x_cross(j))
        for j in range(1, gy):
            give(at, slot(0, gy - j, 1) + at, end - at, every, sem, y_cross(j))
        give(at, slot(0, 0, 1) + at, end - at, every, 0, sibling)

    def ag_forward(g):
        at, end = split(g) if g >= 0 else (0, 1)
        n, sem = end - at, sem_of(g)
        if n == 0:
            return
        if gx + gy > 2:
            arrived(all_ref.at[pl.ds(0, (gx + gy - 2) * n)], ag_sems.at[sem])
        for dx in range(1, gx):
            for j in range(1, gy):
                give(slot(dx, 0, 1) + at, slot(dx, gy - j, 1) + at, n, front, sem + 1, y_peer(j))
                if g == PIECES - 1:
                    give(slot(dx, 0, 1) + at, slot(dx, gy - j, 0) + at, n, front, cross, y_cross(j))
        for dy in range(1, gy):
            for j in range(1, gx):
                give(slot(0, dy, 1) + at, slot(gx - j, dy, 1) + at, n, back, sem + 1, x_peer(j))
                if g == PIECES - 1:
                    give(slot(0, dy, 1) + at, slot(gx - j, dy, 0) + at, n, back, cross, x_cross(j))
        for dx in range(1, gx):
            give(slot(dx, 0, 1) + at, slot(dx, 0, 0) + at, n, every, 0, sibling)
        for dy in range(1, gy):
            give(slot(0, dy, 1) + at, slot(0, dy, 0) + at, n, every, 0, sibling)

    def ag_core(g):
        at, end = split(g) if g >= 0 else (0, 1)
        n, sem = end - at, sem_of(g)
        count = (gx - 1) * (gy - 1) * n
        if count:
            arrived(all_ref.at[pl.ds(0, count)], ag_sems.at[sem + 1])
        if g == PIECES - 1:
            return
        for dx in range(1, gx):
            for dy in range(1, gy):
                give(slot(dx, dy, 1) + at, slot(dx, dy, 0) + at, n, every, 1, sibling)

    def ag_own():
        own_ref.wait()
        for j in range(1, gz):
            give(0, gz - j, 1, every, 2, z_peer(j))
        ag_direct(-1)

    def ag_z():
        if gz > 1:
            arrived(all_ref.at[pl.ds(1, gz - 1)], ag_sems.at[2])

    diag = (gx - 1) * (gy - 1) * gz
    early, late = [], []
    for dc in range(2):
        for dx in range(gx):
            for dy in range(gy):
                runs = late if dx and dy else early
                at = slot(dx, dy, dc)
                if runs and runs[-1][1] == at and at != half:
                    runs[-1] = (runs[-1][0], at + gz)
                else:
                    runs.append((at, at + gz))

    for copy in metas:
        copy.wait()
    angle = orient_ref[...].astype(jnp.float32) * (2.0 * math.pi / ORIENTS)
    bins = tilt_ref[...].astype(jnp.float32)
    low_end = -(40.0 + 1.5 * bins[0:1]) * (math.pi / 180.0)
    high_end = (40.0 + 1.5 * bins[1:2]) * (math.pi / 180.0)
    sin_a, cos_a = column(jnp.sin(angle)), column(jnp.cos(angle))
    cos_c = column(jnp.cos(low_end + high_end))
    sin_c = column(jnp.sin(low_end + high_end))
    cos_w = column(jnp.cos(high_end - low_end))
    cls_row = cls_ref[...].astype(jnp.float32)
    cls_col = column(cls_row)

    def log2(n):
        return n.bit_length() - 1

    row = lax.broadcasted_iota(jnp.int32, (classes, 1), 0)

    def ids_of(order, flip):
        left, at = row, {}
        for dim in reversed(order):
            at[dim] = left & (sizes[dim] - 1)
            left = lax.shift_right_logical(left, log2(sizes[dim]))
        return device((at["x"] + x) & (gx - 1), (at["y"] + y) & (gy - 1), (at["z"] + z) & (gz - 1), (left + core + flip) & 1)

    ids = ids_of("xyz", 0)
    onehot = {}
    for order in ORDERS:
        if order not in onehot:
            onehot[order] = jnp.where(ids_of(order, 1).astype(jnp.float32) == cls_row, 1.0, 0.0).astype(jnp.bfloat16)
    sums = {"wedge": jnp.zeros((rows, 1), jnp.float32), "power": jnp.zeros((rows, 1), jnp.float32)}

    def parts(first, size):
        width = max(0, min(size, coef - first))
        pieces = []
        if width:
            both = part[:, :, first:first + width].astype(jnp.float32)
            pieces.append(jnp.swapaxes(both, 0, 1))
        if width < size:
            pieces.append(jnp.zeros((2, rows, size - width), jnp.float32))
        both = jnp.concatenate(pieces, axis=2) if len(pieces) > 1 else pieces[0]
        return both[0], both[1]

    def wedges(first, size):
        freq_x, freq_y, freq_z, index = frequencies(first, size)
        along = freq_y * cos_a - freq_x * sin_a
        along_sq = along * along
        z_sq = freq_z * freq_z
        scale = 1.0 / (along_sq + (z_sq + 1.0))
        value = ((along_sq - z_sq) * cos_c - (2.0 * along * freq_z) * sin_c) * scale - cos_w
        wedge = 1.0 / (1.0 + jnp.exp(value * (-GAIN)))
        inside = wedge if first + size <= coef else jnp.where(index < coef, wedge, 0.0)
        sums["wedge"] = sums["wedge"] + jnp.sum(inside, axis=1, keepdims=True)
        return wedge

    def compute(t):
        span = spans[t]
        if t % 2 == 0:
            part_copies[t // 2].wait()
        for at in range(0, span, SUB):
            first = starts[t] + at
            size = min(SUB, span - at)
            wedge = wedges(first, size)
            real, imag = parts(first, size)
            sums["power"] = sums["power"] + jnp.sum(wedge * (real * real + imag * imag), axis=1, keepdims=True)
            data[t][:, at:at + size] = (wedge * real).astype(jnp.bfloat16)
            data[t][:, span + at:span + at + size] = (wedge * imag).astype(jnp.bfloat16)
            data[t][:, 2 * span + at:2 * span + at + size] = (wedge * wedge).astype(jnp.bfloat16)
            low[:, first:first + size] = wedge.astype(jnp.bfloat16)
        for q in range(3):
            cols = slice(q * span, (q + 1) * span)
            both = jnp.dot(onehot[ORDERS[t]], data[t][:, cols], preferred_element_type=jnp.float32)
            send_core[t][:, cols] = both[half:].astype(jnp.bfloat16)
            mine[t][:, cols] = both[:half]

    def cores(t):
        push(send_core[t], recv_core[t], send_sems.at[1], core_sems.at[t // 2], sibling)

    def fold(line):
        wide = line.shape[1]
        return jnp.concatenate([line[:, :wide // 2], line[:, wide // 2:]], axis=0)

    def taken(t, k):
        if k < 0:
            if t % 2 == 0:
                arrived(core_pairs[t // 2], core_sems.at[t // 2])
            return mine[t][...] + recv_core[t][...].astype(jnp.float32)
        n = sizes[ORDERS[t][k]]
        lines = math.prod(sizes[dim] for dim in ORDERS[t][k + 1:])
        recv = hop_recvs[3 * t + k]
        if k == 1 or n > 1:
            arrived(recv, hop_sems.at[3 * t + k])
        if k == 1:
            piece = recv[0].astype(jnp.float32)
            for j in range(1, n):
                piece = piece + recv[j].astype(jnp.float32)
            return piece
        piece = mine[t][:lines]
        if lines == 1:
            piece = fold(piece)
        for j in range(1, n):
            piece = piece + recv[j - 1].astype(jnp.float32)
        return piece

    def hop(t, k):
        dim = ORDERS[t][k]
        lines = math.prod(sizes[dim] for dim in ORDERS[t][k + 1:])
        piece = taken(t, k - 1)
        send, recv = hop_sends[3 * t + k], hop_recvs[3 * t + k]
        for j in range(0 if k == 1 else 1, sizes[dim]):
            part_of = piece[j * lines:(j + 1) * lines]
            if lines == 1:
                part_of = fold(part_of)
            at = j if k == 1 else j - 1
            send[at] = part_of.astype(jnp.bfloat16)
            peer = sibling if j == 0 else (cross_of if k == 1 else peer_of)[dim](j)
            sem = 4 if j == 0 else 2
            push(send.at[at], recv.at[at], send_sems.at[sem], hop_sems.at[3 * t + k], peer)
        if k != 1:
            mine[t][:lines] = piece[:lines]

    def first(t):
        hop(t, 0)

    def second(t):
        hop(t, 1)

    def third(t):
        hop(t, 2)

    reach = small_send.shape[2] // 2
    stages = [(1, lambda j: sibling)] + [(sizes[dim] - 1, (peer_of, cross_of, peer_of)[k][dim]) for k, dim in enumerate(SMALL)]

    def small_start():
        lane = lax.broadcasted_iota(jnp.int32, (rows, reach), 1).astype(jnp.float32)
        hits = jnp.where(lane == cls_col, 1.0, 0.0)
        small_send[0, :, :reach] = jnp.sum(hits, axis=0, keepdims=True)
        small_send[0, :, reach:] = jnp.sum(hits * sums["wedge"], axis=0, keepdims=True)
        small_push(0)

    def small_push(k):
        at = sum(n for n, _ in stages[:k])
        for j in range(stages[k][0]):
            push(small_send.at[k], small_recv.at[at + j], send_sems.at[3], small_sems.at[k], stages[k][1](j + 1))

    def small_take(k):
        at, n = sum(n for n, _ in stages[:k]), stages[k][0]
        tally = small_send[k]
        if n:
            arrived(small_recv.at[pl.ds(at, n)], small_sems.at[k])
        for j in range(n):
            tally = tally + small_recv[at + j]
        return tally

    def small_next(k):
        small_send[k + 1] = small_take(k)
        small_push(k + 1)

    nt = (((1,), (1,)), ((), ()))
    table = []

    def position(at):
        before = 0
        for begin, end in early + late:
            if begin <= at < end:
                return before + at - begin
            before += end - begin

    order = jnp.concatenate([ids[begin:end] for begin, end in early + late], axis=0)

    def prepare(runs):
        for begin, end in runs:
            lines = slice(begin, end)
            for t in range(CHUNKS):
                cols = slice(starts[t], starts[t] + widths[t])
                both = jnp.swapaxes(all_ref[lines, :, cols].astype(jnp.float32), 0, 1)
                real, imag = both[0], both[1]
                to = slice(position(begin), position(begin) + end - begin)
                ready[0, to, cols] = real.astype(jnp.bfloat16)
                ready[1, to, cols] = imag.astype(jnp.bfloat16)
                ready[2, to, cols] = (real * real + imag * imag).astype(jnp.bfloat16)

    def score(begin, end):
        power = sums["power"]
        for at in range(begin, end, 32):
            lines = slice(at, min(at + 32, end))
            group = lines.stop - lines.start
            inter = jnp.zeros((rows, group), jnp.float32)
            energy = jnp.zeros((rows, group), jnp.float32)
            for t in range(CHUNKS):
                width, span = widths[t], spans[t]
                cols = slice(starts[t], starts[t] + width)
                inter = inter + lax.dot_general(data[t][:, :width], ready[0, lines, cols], nt, preferred_element_type=jnp.float32)
                inter = inter + lax.dot_general(data[t][:, span:span + width], ready[1, lines, cols], nt, preferred_element_type=jnp.float32)
                energy = energy + lax.dot_general(low[:, cols], ready[2, lines, cols], nt, preferred_element_type=jnp.float32)
            value = inter / (math.sqrt(coef) * jnp.sqrt((energy / coef + EPS) * (power / coef + EPS)))
            lane = lax.broadcasted_iota(jnp.int32, (group, classes), 1)
            place = jnp.where(order[lines] == lane, 1.0, 0.0)
            table.append(jnp.dot(value, place, precision=lax.Precision.HIGHEST, preferred_element_type=jnp.float32))

    groups = [(at, at + gz) for begin, end in early for at in range(begin, end, gz)]

    def merged(runs):
        out = []
        for begin, end in runs:
            if out and out[-1][1] == begin and begin != half:
                out[-1] = (out[-1][0], end)
            else:
                out.append((begin, end))
        return out

    def prepare_near():
        prepare(merged([g for g in groups if (g[0] < half) == (g[0] % half == 0)]))

    def prepare_far():
        arrived(all_ref.at[pl.ds(0, half - diag)], ag_sems.at[0])
        prepare(merged([g for g in groups if (g[0] < half) != (g[0] % half == 0)]))

    def score_late():
        last = (gx - 1) * (gy - 1) * (gz - split(PIECES - 1)[0])
        if diag > last:
            arrived(all_ref.at[pl.ds(0, diag - last)], ag_sems.at[1])
        if last:
            arrived(all_ref.at[pl.ds(0, last)], ag_sems.at[cross])
        prepare(late)
        score(classes - 2 * diag, classes)
        scores_ref[...] = sum(table[1:], table[0])

    floors = []

    def counts():
        tally = small_take(3)
        load_ref[...] = tally[:, :classes] * classes / total
        lane = lax.broadcasted_iota(jnp.int32, (1, reach), 1)
        wedge_total = jnp.sum(jnp.where(lane == me, tally[:, reach:], 0.0), axis=1, keepdims=True)
        floors.append(TAU * (wedge_total / coef + 1.0))

    def means(t):
        whole = taken(t, 2)
        flat = jnp.concatenate([whole[0:1], whole[1:2]], axis=1)
        span, width, start = spans[t], widths[t], starts[t]
        scale = 1.0 / (flat[:, 2 * span:2 * span + width] + floors[0])
        for q in range(2):
            means_ref[0, q:q + 1, start:start + width] = flat[:, q * span:q * span + width] * scale

    compute(0)
    pl.semaphore_wait(barrier, len(peers))
    ag_own()
    cores(0)
    compute(1)
    cores(1)
    compute(2)
    cores(2)
    compute(3)
    cores(3)
    hop(0, 0)
    hop(1, 0)
    compute(4)
    cores(4)
    compute(5)
    cores(5)
    small_start()
    hop(2, 0)
    hop(3, 0)
    small_next(0)
    hop(4, 0)
    hop(5, 0)
    ag_forward(-1)
    hop(0, 1)
    hop(1, 1)
    ag_z()
    ag_direct(0)
    ag_direct(1)
    ag_direct(2)
    hop(2, 1)
    hop(3, 1)
    small_next(1)
    hop(4, 1)
    hop(5, 1)
    ag_core(-1)
    ag_forward(0)
    ag_forward(1)
    ag_forward(2)
    small_next(2)
    hop(2, 2)
    hop(3, 2)
    hop(4, 2)
    hop(5, 2)
    hop(0, 2)
    hop(1, 2)
    prepare_near()
    ag_core(0)
    ag_core(1)
    prepare_far()
    score(0, classes - 2 * diag)
    ag_core(2)
    score_late()
    counts()
    means(0)
    means(1)
    means(2)
    means(3)
    means(4)
    means(5)

    whole_of(all_ref.at[pl.ds(0, classes - 1)], send_sems.at[0]).wait_send()
    whole_of(ready.at[:, :half, :], send_sems.at[1]).wait_send()
    whole_of(all_ref.at[pl.ds(0, classes - 2), :, :3 * sum(spans) // 4], send_sems.at[2]).wait_send()
    whole_of(small_recv, send_sems.at[3]).wait_send()
    kept = sum(3 * spans[t] * sizes[ORDERS[t][2]] for t in range(CHUNKS)) // (2 * LANES)
    lines = next(n for n in range(classes, 0, -1) if kept % n == 0 and kept // n * LANES <= coef)
    whole_of(all_ref.at[pl.ds(0, lines), :, :kept // lines * LANES], send_sems.at[4]).wait_send()


def finish(*arrays):
    n = len(arrays)

    def put(*refs):
        sems = refs[2 * n]
        copies = [pltpu.make_async_copy(refs[i], refs[n + i], sems.at[i]) for i in range(n)]
        for copy in copies:
            copy.start()
        for copy in copies:
            copy.wait()

    scores, means, load = pl.pallas_call(
        put,
        out_shape=tuple(jax.ShapeDtypeStruct(a.shape, a.dtype) for a in arrays),
        in_specs=[pl.BlockSpec(memory_space=pltpu.VMEM)] * n,
        out_specs=(pl.BlockSpec(memory_space=pltpu.HBM),) * n,
        scratch_shapes=[pltpu.SemaphoreType.DMA((n,))],
        compiler_params=pltpu.CompilerParams(vmem_limit_bytes=1024 * 1024),
    )(*arrays)
    return (scores, means, load[0])


def body(particles, references, assignment, orientation, tilt_range):
    part_rows = particles.shape[0]
    coef = particles.shape[2]
    devices = lax.axis_size("dom")
    classes = references.shape[0] * devices
    assert references.shape[0] == 1
    gx, gy, gz = factor(devices)
    total = part_rows * devices
    spans = spans_of(coef)
    padded = sum(spans)
    width = 2 * (-(-classes // LANES) * LANES)
    half = classes // 2

    vmem = pl.BlockSpec(memory_space=pltpu.VMEM)
    hbm = pl.BlockSpec(memory_space=pltpu.HBM)
    dma = pltpu.SemaphoreType.DMA
    bf16, f32, i32 = jnp.bfloat16, jnp.float32, jnp.int32

    sizes = {"x": gx, "y": gy, "z": gz}
    hops = []
    for order, span in zip(ORDERS, spans):
        wide = 3 * span
        for k, dim in enumerate(order):
            lines = math.prod(sizes[d] for d in order[k + 1:])
            shape = (lines, wide) if lines > 1 else (2, wide // 2)
            hops.append(((max(1, sizes[dim] - (k != 1)), *shape), bf16))
    buffers = [
        ((part_rows, 2, coef), bf16),
        ((1, part_rows), i32),
        ((1, part_rows), i32),
        ((2, part_rows), i32),
        ((part_rows, padded), bf16),
        ((classes, 2, coef), bf16),
        ((3, classes, padded), bf16),
        ((4, 1, width), f32),
        ((gx + gy + gz - 2, 1, width), f32),
        *hops, *hops,
        *[((part_rows, 3 * span), bf16) for span in spans],
        *[((half, 3 * span), f32) for span in spans],
        *[((half, 3 * span), bf16) for span in spans],
        *[((2, half, 3 * span), bf16) for span in spans[::2]],
    ]
    held = sum(math.prod(shape) * jnp.dtype(kind).itemsize for shape, kind in buffers)
    limit = min(60, held // 2**20 + 8) * 2**20
    scores, means, load = pl.pallas_call(
        functools.partial(kernel, gx, gy, gz, spans, coef, total),
        out_shape=(
            jax.ShapeDtypeStruct((part_rows, classes), f32),
            jax.ShapeDtypeStruct((1, 2, coef), f32),
            jax.ShapeDtypeStruct((1, classes), f32),
        ),
        in_specs=[hbm] * 5,
        out_specs=(vmem, vmem, vmem),
        scratch_shapes=[pltpu.VMEM(shape, kind) for shape, kind in buffers] + [
            dma((4 + CHUNKS // 2,)), dma((3 + 2 * (PIECES + 1) + 1,)), dma((CHUNKS // 2,)), dma((3 * CHUNKS,)), dma((4,)), dma((5,)),
        ],
        compiler_params=pltpu.CompilerParams(
            collective_id=0, has_side_effects=True, vmem_limit_bytes=limit
        ),
    )(*[
        pltpu.with_memory_space_constraint(v, pltpu.HBM)
        for v in (particles, references, assignment.reshape(1, part_rows), orientation[None, :], tilt_range)
    ])
    return finish(scores, means, load)


def solution(mesh):
    in_specs = (
        P("dom", None, None),
        P("dom", None, None),
        P("dom", None),
        P("dom"),
        P(None, "dom"),
    )
    out_specs = (P("dom", None), P("dom", None, None), P())
    return jax.shard_map(body, mesh=mesh, in_specs=in_specs, out_specs=out_specs, check_vma=False)
```

```python
import functools
import math

import jax
import jax.numpy as jnp
from jax import lax
from jax.experimental import pallas as pl
from jax.experimental.pallas import tpu as pltpu
from jax.sharding import PartitionSpec as P

GRID = 24
ORIENTS = 36
EPS = 1e-06
GAIN = 6.0
TAU = 0.5
LANES = 128
MESH = pl.DeviceIdType.MESH

SHARES = (14, 14, 8, 8, 8, 8)
CHUNKS = len(SHARES)
SUB = 640
ORDERS = ("xzy", "yzx", "xyz", "yxz", "xyz", "yxz")
SMALL = "xyz"
PIECES = 3


def factor(devices):
    chips = devices // 2
    log = chips.bit_length() - 1
    gx = 1 << (log // 3)
    gy = 1 << ((log - log // 3) // 2)
    return gx, gy, chips // (gx * gy)


def spans_of(coef):
    unit = sum(SHARES)
    pairs = -(-coef // (4 * LANES)) * 2
    ends = [sum(SHARES[:t + 1]) * pairs // unit for t in range(CHUNKS)]
    return [(end - start) * 2 * LANES for start, end in zip([0] + ends, ends)]


def column(row):
    rows = row.shape[1]
    line = lax.broadcasted_iota(jnp.int32, (rows, rows), 0)
    lane = lax.broadcasted_iota(jnp.int32, (rows, rows), 1)
    return jnp.sum(jnp.where(line == lane, row, 0.0), axis=1, keepdims=True)


def frequencies(first, width):
    index = (lax.broadcasted_iota(jnp.int32, (1, width), 1) + first).astype(jnp.float32)
    plane = jnp.floor((index + 0.5) * (1.0 / (GRID * GRID)))
    rest = index - plane * (GRID * GRID)
    col_x = jnp.floor((rest + 0.5) * (1.0 / GRID))
    col_z = rest - col_x * GRID
    freq_x = jnp.where(col_x >= GRID // 2, col_x - GRID, col_x)
    freq_z = jnp.where(col_z >= GRID // 2, col_z - GRID, col_z)
    return freq_x, plane, freq_z, index


def kernel(
    gx, gy, gz, spans, coef, total,
    part_hbm, ref_hbm, cls_hbm, orient_hbm, tilt_hbm,
    scores_ref, means_ref, load_ref,
    part, cls_ref, orient_ref, tilt_ref,
    low, all_ref, ready, small_send, small_recv, *rest,
):
    hop_sends, hop_recvs = rest[:3 * CHUNKS], rest[3 * CHUNKS:6 * CHUNKS]
    data, mine, send_core, recv_core = (rest[k * CHUNKS:(k + 1) * CHUNKS] for k in range(6, 10))
    extra = CHUNKS // 2
    core_pairs = recv_core[:CHUNKS // 2]
    recv_core = [core_pairs[t // 2].at[t % 2] for t in range(CHUNKS)]
    in_sems, ag_sems, core_sems, hop_sems, small_sems, send_sems = rest[10 * CHUNKS - extra:]
    starts = [sum(spans[:t]) for t in range(CHUNKS)]
    widths = [max(0, min(spans[t], coef - starts[t])) for t in range(CHUNKS)]
    me = lax.axis_index("dom")
    core = lax.rem(me, 2)
    chip = me // 2
    x = lax.rem(chip, gx)
    y = lax.rem(chip // gx, gy)
    z = chip // (gx * gy)
    sibling = me + 1 - 2 * core
    classes = 2 * gx * gy * gz
    half = classes // 2
    rows = part.shape[0]
    cut = coef // 2 // LANES * LANES

    def device(x_at, y_at, z_at, c_at):
        return ((z_at * gy + y_at) * gx + x_at) * 2 + c_at

    def x_peer(j):
        return device(lax.rem(x + j, gx), y, z, core)

    def y_peer(j):
        return device(x, lax.rem(y + j, gy), z, core)

    def x_cross(j):
        return device(lax.rem(x + j, gx), y, z, 1 - core)

    def y_cross(j):
        return device(x, lax.rem(y + j, gy), z, 1 - core)

    def z_cross(j):
        return device(x, y, lax.rem(z + j, gz), 1 - core)

    def z_peer(j):
        return device(x, y, lax.rem(z + j, gz), core)

    sizes = {"x": gx, "y": gy, "z": gz}
    peer_of = {"x": x_peer, "y": y_peer, "z": z_peer}
    cross_of = {"x": x_cross, "y": y_cross, "z": z_cross}

    def fetch(src, dst, at):
        copy = pltpu.make_async_copy(src, dst, in_sems.at[at])
        copy.start()
        return copy

    barrier = pltpu.get_barrier_semaphore()
    peers = [sibling]
    peers += [x_peer(j) for j in range(1, gx)]
    peers += [y_peer(j) for j in range(1, gy)]
    peers += [z_peer(j) for j in range(1, gz)]
    peers += [x_cross(j) for j in range(1, gx)]
    peers += [y_cross(j) for j in range(1, gy)]
    peers += [z_cross(j) for j in range(1, gz)]
    for peer in peers:
        pl.semaphore_signal(barrier, inc=1, device_id=(peer,), device_id_type=MESH)
    metas = [
        fetch(orient_hbm, orient_ref, 1),
        fetch(tilt_hbm, tilt_ref, 2),
        fetch(cls_hbm, cls_ref, 3),
    ]
    own_ref = fetch(ref_hbm.at[0], all_ref.at[0], 0)
    part_copies = []
    for t in range(0, CHUNKS, 2):
        cols = pl.ds(starts[t], widths[t] + widths[t + 1])
        part_copies.append(fetch(part_hbm.at[:, :, cols], part.at[:, :, cols], 4 + t // 2))

    def push(src, dst, send_sem, recv_sem, target):
        pltpu.make_async_remote_copy(
            src_ref=src, dst_ref=dst, send_sem=send_sem, recv_sem=recv_sem,
            device_id=(target,), device_id_type=MESH,
        ).start()

    def whole_of(ref, sem):
        return pltpu.make_async_remote_copy(
            src_ref=ref, dst_ref=ref, send_sem=sem, recv_sem=sem,
            device_id=(sibling,), device_id_type=MESH,
        )

    def arrived(ref, sem):
        whole_of(ref, sem).wait_recv()

    def slot(dx, dy, dc):
        return ((dc * gx + dx) * gy + dy) * gz

    def give(src_slot, dst_slot, n, lanes, at, target):
        src = all_ref.at[pl.ds(src_slot, n), :, lanes]
        dst = all_ref.at[pl.ds(dst_slot, n), :, lanes]
        push(src, dst, send_sems.at[0], ag_sems.at[at], target)

    every = slice(0, coef)
    front, back = slice(0, cut), slice(cut, coef)

    def split(g):
        return 1 + g * (gz - 1) // PIECES, 1 + (g + 1) * (gz - 1) // PIECES

    def sem_of(g):
        return 3 + 2 * (g + 1)

    cross = sem_of(PIECES)

    def ag_direct(g):
        at, end = split(g) if g >= 0 else (0, 1)
        sem = sem_of(g)
        if at == end:
            return
        for j in range(1, gx):
            give(at, slot(gx - j, 0, 1) + at, end - at, every, sem, x_cross(j))
        for j in range(1, gy):
            give(at, slot(0, gy - j, 1) + at, end - at, every, sem, y_cross(j))
        give(at, slot(0, 0, 1) + at, end - at, every, 0, sibling)

    def ag_forward(g):
        at, end = split(g) if g >= 0 else (0, 1)
        n, sem = end - at, sem_of(g)
        if n == 0:
            return
        if gx + gy > 2:
            arrived(all_ref.at[pl.ds(0, (gx + gy - 2) * n)], ag_sems.at[sem])
        for dx in range(1, gx):
            for j in range(1, gy):
                give(slot(dx, 0, 1) + at, slot(dx, gy - j, 1) + at, n, front, sem + 1, y_peer(j))
                if g == PIECES - 1:
                    give(slot(dx, 0, 1) + at, slot(dx, gy - j, 0) + at, n, front, cross, y_cross(j))
        for dy in range(1, gy):
            for j in range(1, gx):
                give(slot(0, dy, 1) + at, slot(gx - j, dy, 1) + at, n, back, sem + 1, x_peer(j))
                if g == PIECES - 1:
                    give(slot(0, dy, 1) + at, slot(gx - j, dy, 0) + at, n, back, cross, x_cross(j))
        for dx in range(1, gx):
            give(slot(dx, 0, 1) + at, slot(dx, 0, 0) + at, n, every, 0, sibling)
        for dy in range(1, gy):
            give(slot(0, dy, 1) + at, slot(0, dy, 0) + at, n, every, 0, sibling)

    def ag_core(g):
        at, end = split(g) if g >= 0 else (0, 1)
        n, sem = end - at, sem_of(g)
        count = (gx - 1) * (gy - 1) * n
        if count:
            arrived(all_ref.at[pl.ds(0, count)], ag_sems.at[sem + 1])
        if g == PIECES - 1:
            return
        for dx in range(1, gx):
            for dy in range(1, gy):
                give(slot(dx, dy, 1) + at, slot(dx, dy, 0) + at, n, every, 1, sibling)

    def ag_own():
        own_ref.wait()
        for j in range(1, gz):
            give(0, gz - j, 1, every, 2, z_peer(j))
        ag_direct(-1)

    def ag_z():
        if gz > 1:
            arrived(all_ref.at[pl.ds(1, gz - 1)], ag_sems.at[2])

    diag = (gx - 1) * (gy - 1) * gz
    early, late = [], []
    for dc in range(2):
        for dx in range(gx):
            for dy in range(gy):
                runs = late if dx and dy else early
                at = slot(dx, dy, dc)
                if runs and runs[-1][1] == at and at != half:
                    runs[-1] = (runs[-1][0], at + gz)
                else:
                    runs.append((at, at + gz))

    for copy in metas:
        copy.wait()
    angle = orient_ref[...].astype(jnp.float32) * (2.0 * math.pi / ORIENTS)
    bins = tilt_ref[...].astype(jnp.float32)
    low_end = -(40.0 + 1.5 * bins[0:1]) * (math.pi / 180.0)
    high_end = (40.0 + 1.5 * bins[1:2]) * (math.pi / 180.0)
    sin_a, cos_a = column(jnp.sin(angle)), column(jnp.cos(angle))
    cos_c = column(jnp.cos(low_end + high_end))
    sin_c = column(jnp.sin(low_end + high_end))
    cos_w = column(jnp.cos(high_end - low_end))
    cls_row = cls_ref[...].astype(jnp.float32)
    cls_col = column(cls_row)

    def log2(n):
        return n.bit_length() - 1

    row = lax.broadcasted_iota(jnp.int32, (classes, 1), 0)

    def ids_of(order, flip):
        left, at = row, {}
        for dim in reversed(order):
            at[dim] = left & (sizes[dim] - 1)
            left = lax.shift_right_logical(left, log2(sizes[dim]))
        return device((at["x"] + x) & (gx - 1), (at["y"] + y) & (gy - 1), (at["z"] + z) & (gz - 1), (left + core + flip) & 1)

    ids = ids_of("xyz", 0)
    onehot = {}
    for order in ORDERS:
        if order not in onehot:
            onehot[order] = jnp.where(ids_of(order, 1).astype(jnp.float32) == cls_row, 1.0, 0.0).astype(jnp.bfloat16)
    sums = {"wedge": jnp.zeros((rows, 1), jnp.float32), "power": jnp.zeros((rows, 1), jnp.float32)}

    def parts(first, size):
        width = max(0, min(size, coef - first))
        pieces = []
        if width:
            both = part[:, :, first:first + width].astype(jnp.float32)
            pieces.append(jnp.swapaxes(both, 0, 1))
        if width < size:
            pieces.append(jnp.zeros((2, rows, size - width), jnp.float32))
        both = jnp.concatenate(pieces, axis=2) if len(pieces) > 1 else pieces[0]
        return both[0], both[1]

    def wedges(first, size):
        freq_x, freq_y, freq_z, index = frequencies(first, size)
        along = freq_y * cos_a - freq_x * sin_a
        along_sq = along * along
        z_sq = freq_z * freq_z
        scale = 1.0 / (along_sq + (z_sq + 1.0))
        value = ((along_sq - z_sq) * cos_c - (2.0 * along * freq_z) * sin_c) * scale - cos_w
        wedge = 1.0 / (1.0 + jnp.exp(value * (-GAIN)))
        inside = wedge if first + size <= coef else jnp.where(index < coef, wedge, 0.0)
        sums["wedge"] = sums["wedge"] + jnp.sum(inside, axis=1, keepdims=True)
        return wedge

    def compute(t):
        span = spans[t]
        if t % 2 == 0:
            part_copies[t // 2].wait()
        for at in range(0, span, SUB):
            first = starts[t] + at
            size = min(SUB, span - at)
            wedge = wedges(first, size)
            real, imag = parts(first, size)
            sums["power"] = sums["power"] + jnp.sum(wedge * (real * real + imag * imag), axis=1, keepdims=True)
            data[t][:, at:at + size] = (wedge * real).astype(jnp.bfloat16)
            data[t][:, span + at:span + at + size] = (wedge * imag).astype(jnp.bfloat16)
            data[t][:, 2 * span + at:2 * span + at + size] = (wedge * wedge).astype(jnp.bfloat16)
            low[:, first:first + size] = wedge.astype(jnp.bfloat16)
        for q in range(3):
            cols = slice(q * span, (q + 1) * span)
            both = jnp.dot(onehot[ORDERS[t]], data[t][:, cols], preferred_element_type=jnp.float32)
            send_core[t][:, cols] = both[half:].astype(jnp.bfloat16)
            mine[t][:, cols] = both[:half]

    def cores(t):
        push(send_core[t], recv_core[t], send_sems.at[1], core_sems.at[t // 2], sibling)

    def fold(line):
        wide = line.shape[1]
        return jnp.concatenate([line[:, :wide // 2], line[:, wide // 2:]], axis=0)

    def taken(t, k):
        if k < 0:
            if t % 2 == 0:
                arrived(core_pairs[t // 2], core_sems.at[t // 2])
            return mine[t][...] + recv_core[t][...].astype(jnp.float32)
        n = sizes[ORDERS[t][k]]
        lines = math.prod(sizes[dim] for dim in ORDERS[t][k + 1:])
        recv = hop_recvs[3 * t + k]
        if k == 1 or n > 1:
            arrived(recv, hop_sems.at[3 * t + k])
        if k == 1:
            piece = recv[0].astype(jnp.float32)
            for j in range(1, n):
                piece = piece + recv[j].astype(jnp.float32)
            return piece
        piece = mine[t][:lines]
        if lines == 1:
            piece = fold(piece)
        for j in range(1, n):
            piece = piece + recv[j - 1].astype(jnp.float32)
        return piece

    def hop(t, k):
        dim = ORDERS[t][k]
        lines = math.prod(sizes[dim] for dim in ORDERS[t][k + 1:])
        piece = taken(t, k - 1)
        send, recv = hop_sends[3 * t + k], hop_recvs[3 * t + k]
        for j in range(0 if k == 1 else 1, sizes[dim]):
            part_of = piece[j * lines:(j + 1) * lines]
            if lines == 1:
                part_of = fold(part_of)
            at = j if k == 1 else j - 1
            send[at] = part_of.astype(jnp.bfloat16)
            peer = sibling if j == 0 else (cross_of if k == 1 else peer_of)[dim](j)
            sem = 4 if j == 0 else 2
            push(send.at[at], recv.at[at], send_sems.at[sem], hop_sems.at[3 * t + k], peer)
        if k != 1:
            mine[t][:lines] = piece[:lines]

    def first(t):
        hop(t, 0)

    def second(t):
        hop(t, 1)

    def third(t):
        hop(t, 2)

    reach = small_send.shape[2] // 2
    stages = [(1, lambda j: sibling)] + [(sizes[dim] - 1, (peer_of, cross_of, peer_of)[k][dim]) for k, dim in enumerate(SMALL)]

    def small_start():
        lane = lax.broadcasted_iota(jnp.int32, (rows, reach), 1).astype(jnp.float32)
        hits = jnp.where(lane == cls_col, 1.0, 0.0)
        small_send[0, :, :reach] = jnp.sum(hits, axis=0, keepdims=True)
        small_send[0, :, reach:] = jnp.sum(hits * sums["wedge"], axis=0, keepdims=True)
        small_push(0)

    def small_push(k):
        at = sum(n for n, _ in stages[:k])
        for j in range(stages[k][0]):
            push(small_send.at[k], small_recv.at[at + j], send_sems.at[3], small_sems.at[k], stages[k][1](j + 1))

    def small_take(k):
        at, n = sum(n for n, _ in stages[:k]), stages[k][0]
        tally = small_send[k]
        if n:
            arrived(small_recv.at[pl.ds(at, n)], small_sems.at[k])
        for j in range(n):
            tally = tally + small_recv[at + j]
        return tally

    def small_next(k):
        small_send[k + 1] = small_take(k)
        small_push(k + 1)

    nt = (((1,), (1,)), ((), ()))
    table = []

    def position(at):
        before = 0
        for begin, end in early + late:
            if begin <= at < end:
                return before + at - begin
            before += end - begin

    order = jnp.concatenate([ids[begin:end] for begin, end in early + late], axis=0)

    def prepare(runs):
        for begin, end in runs:
            lines = slice(begin, end)
            for t in range(CHUNKS):
                cols = slice(starts[t], starts[t] + widths[t])
                both = jnp.swapaxes(all_ref[lines, :, cols].astype(jnp.float32), 0, 1)
                real, imag = both[0], both[1]
                to = slice(position(begin), position(begin) + end - begin)
                ready[0, to, cols] = real.astype(jnp.bfloat16)
                ready[1, to, cols] = imag.astype(jnp.bfloat16)
                ready[2, to, cols] = (real * real + imag * imag).astype(jnp.bfloat16)

    def score(begin, end):
        power = sums["power"]
        for at in range(begin, end, 32):
            lines = slice(at, min(at + 32, end))
            group = lines.stop - lines.start
            inter = jnp.zeros((rows, group), jnp.float32)
            energy = jnp.zeros((rows, group), jnp.float32)
            for t in range(CHUNKS):
                width, span = widths[t], spans[t]
                cols = slice(starts[t], starts[t] + width)
                inter = inter + lax.dot_general(data[t][:, :width], ready[0, lines, cols], nt, preferred_element_type=jnp.float32)
                inter = inter + lax.dot_general(data[t][:, span:span + width], ready[1, lines, cols], nt, preferred_element_type=jnp.float32)
                energy = energy + lax.dot_general(low[:, cols], ready[2, lines, cols], nt, preferred_element_type=jnp.float32)
            value = inter / (math.sqrt(coef) * jnp.sqrt((energy / coef + EPS) * (power / coef + EPS)))
            lane = lax.broadcasted_iota(jnp.int32, (group, classes), 1)
            place = jnp.where(order[lines] == lane, 1.0, 0.0)
            table.append(jnp.dot(value, place, precision=lax.Precision.HIGHEST, preferred_element_type=jnp.float32))

    groups = [(at, at + gz) for begin, end in early for at in range(begin, end, gz)]

    def merged(runs):
        out = []
        for begin, end in runs:
            if out and out[-1][1] == begin and begin != half:
                out[-1] = (out[-1][0], end)
            else:
                out.append((begin, end))
        return out

    def prepare_near():
        prepare(merged([g for g in groups if (g[0] < half) == (g[0] % half == 0)]))

    def prepare_far():
        arrived(all_ref.at[pl.ds(0, half - diag)], ag_sems.at[0])
        prepare(merged([g for g in groups if (g[0] < half) != (g[0] % half == 0)]))

    def score_late():
        last = (gx - 1) * (gy - 1) * (gz - split(PIECES - 1)[0])
        if diag > last:
            arrived(all_ref.at[pl.ds(0, diag - last)], ag_sems.at[1])
        if last:
            arrived(all_ref.at[pl.ds(0, last)], ag_sems.at[cross])
        prepare(late)
        score(classes - 2 * diag, classes)
        scores_ref[...] = sum(table[1:], table[0])

    floors = []

    def counts():
        tally = small_take(3)
        load_ref[...] = tally[:, :classes] * classes / total
        lane = lax.broadcasted_iota(jnp.int32, (1, reach), 1)
        wedge_total = jnp.sum(jnp.where(lane == me, tally[:, reach:], 0.0), axis=1, keepdims=True)
        floors.append(TAU * (wedge_total / coef + 1.0))

    def means(t):
        whole = taken(t, 2)
        flat = jnp.concatenate([whole[0:1], whole[1:2]], axis=1)
        span, width, start = spans[t], widths[t], starts[t]
        scale = 1.0 / (flat[:, 2 * span:2 * span + width] + floors[0])
        for q in range(2):
            means_ref[0, q:q + 1, start:start + width] = flat[:, q * span:q * span + width] * scale

    compute(0)
    pl.semaphore_wait(barrier, len(peers))
    ag_own()
    cores(0)
    compute(1)
    cores(1)
    compute(2)
    cores(2)
    compute(3)
    cores(3)
    hop(0, 0)
    hop(1, 0)
    compute(4)
    cores(4)
    compute(5)
    cores(5)
    small_start()
    hop(2, 0)
    hop(3, 0)
    small_next(0)
    hop(4, 0)
    hop(5, 0)
    ag_forward(-1)
    hop(0, 1)
    hop(1, 1)
    ag_z()
    ag_direct(0)
    ag_direct(1)
    ag_direct(2)
    hop(2, 1)
    hop(3, 1)
    small_next(1)
    hop(4, 1)
    hop(5, 1)
    ag_forward(0)
    ag_forward(1)
    ag_forward(2)
    small_next(2)
    hop(2, 2)
    hop(3, 2)
    hop(4, 2)
    hop(5, 2)
    ag_core(-1)
    hop(0, 2)
    hop(1, 2)
    prepare_near()
    ag_core(0)
    prepare_far()
    score(0, classes - 2 * diag)
    ag_core(1)
    ag_core(2)
    score_late()
    counts()
    means(0)
    means(1)
    means(2)
    means(3)
    means(4)
    means(5)

    whole_of(all_ref.at[pl.ds(0, classes - 1)], send_sems.at[0]).wait_send()
    whole_of(ready.at[:, :half, :], send_sems.at[1]).wait_send()
    whole_of(all_ref.at[pl.ds(0, classes - 2), :, :3 * sum(spans) // 4], send_sems.at[2]).wait_send()
    whole_of(small_recv, send_sems.at[3]).wait_send()
    kept = sum(3 * spans[t] * sizes[ORDERS[t][2]] for t in range(CHUNKS)) // (2 * LANES)
    lines = next(n for n in range(classes, 0, -1) if kept % n == 0 and kept // n * LANES <= coef)
    whole_of(all_ref.at[pl.ds(0, lines), :, :kept // lines * LANES], send_sems.at[4]).wait_send()


def finish(*arrays):
    n = len(arrays)

    def put(*refs):
        sems = refs[2 * n]
        copies = [pltpu.make_async_copy(refs[i], refs[n + i], sems.at[i]) for i in range(n)]
        for copy in copies:
            copy.start()
        for copy in copies:
            copy.wait()

    scores, means, load = pl.pallas_call(
        put,
        out_shape=tuple(jax.ShapeDtypeStruct(a.shape, a.dtype) for a in arrays),
        in_specs=[pl.BlockSpec(memory_space=pltpu.VMEM)] * n,
        out_specs=(pl.BlockSpec(memory_space=pltpu.HBM),) * n,
        scratch_shapes=[pltpu.SemaphoreType.DMA((n,))],
        compiler_params=pltpu.CompilerParams(vmem_limit_bytes=1024 * 1024),
    )(*arrays)
    return (scores, means, load[0])


def body(particles, references, assignment, orientation, tilt_range):
    part_rows = particles.shape[0]
    coef = particles.shape[2]
    devices = lax.axis_size("dom")
    classes = references.shape[0] * devices
    assert references.shape[0] == 1
    gx, gy, gz = factor(devices)
    total = part_rows * devices
    spans = spans_of(coef)
    padded = sum(spans)
    width = 2 * (-(-classes // LANES) * LANES)
    half = classes // 2

    vmem = pl.BlockSpec(memory_space=pltpu.VMEM)
    hbm = pl.BlockSpec(memory_space=pltpu.HBM)
    dma = pltpu.SemaphoreType.DMA
    bf16, f32, i32 = jnp.bfloat16, jnp.float32, jnp.int32

    sizes = {"x": gx, "y": gy, "z": gz}
    hops = []
    for order, span in zip(ORDERS, spans):
        wide = 3 * span
        for k, dim in enumerate(order):
            lines = math.prod(sizes[d] for d in order[k + 1:])
            shape = (lines, wide) if lines > 1 else (2, wide // 2)
            hops.append(((max(1, sizes[dim] - (k != 1)), *shape), bf16))
    buffers = [
        ((part_rows, 2, coef), bf16),
        ((1, part_rows), i32),
        ((1, part_rows), i32),
        ((2, part_rows), i32),
        ((part_rows, padded), bf16),
        ((classes, 2, coef), bf16),
        ((3, classes, padded), bf16),
        ((4, 1, width), f32),
        ((gx + gy + gz - 2, 1, width), f32),
        *hops, *hops,
        *[((part_rows, 3 * span), bf16) for span in spans],
        *[((half, 3 * span), f32) for span in spans],
        *[((half, 3 * span), bf16) for span in spans],
        *[((2, half, 3 * span), bf16) for span in spans[::2]],
    ]
    held = sum(math.prod(shape) * jnp.dtype(kind).itemsize for shape, kind in buffers)
    limit = min(60, held // 2**20 + 8) * 2**20
    scores, means, load = pl.pallas_call(
        functools.partial(kernel, gx, gy, gz, spans, coef, total),
        out_shape=(
            jax.ShapeDtypeStruct((part_rows, classes), f32),
            jax.ShapeDtypeStruct((1, 2, coef), f32),
            jax.ShapeDtypeStruct((1, classes), f32),
        ),
        in_specs=[hbm] * 5,
        out_specs=(vmem, vmem, vmem),
        scratch_shapes=[pltpu.VMEM(shape, kind) for shape, kind in buffers] + [
            dma((4 + CHUNKS // 2,)), dma((3 + 2 * (PIECES + 1) + 1,)), dma((CHUNKS // 2,)), dma((3 * CHUNKS,)), dma((4,)), dma((5,)),
        ],
        compiler_params=pltpu.CompilerParams(
            collective_id=0, has_side_effects=True, vmem_limit_bytes=limit
        ),
    )(*[
        pltpu.with_memory_space_constraint(v, pltpu.HBM)
        for v in (particles, references, assignment.reshape(1, part_rows), orientation[None, :], tilt_range)
    ])
    return finish(scores, means, load)


def solution(mesh):
    in_specs = (
        P("dom", None, None),
        P("dom", None, None),
        P("dom", None),
        P("dom"),
        P(None, "dom"),
    )
    out_specs = (P("dom", None), P("dom", None, None), P())
    return jax.shard_map(body, mesh=mesh, in_specs=in_specs, out_specs=out_specs, check_vma=False)
```

```python
import functools
import math

import jax
import jax.numpy as jnp
from jax import lax
from jax.experimental import pallas as pl
from jax.experimental.pallas import tpu as pltpu
from jax.sharding import PartitionSpec as P

GRID = 24
ORIENTS = 36
EPS = 1e-06
GAIN = 6.0
TAU = 0.5
LANES = 128
MESH = pl.DeviceIdType.MESH

SHARES = (14, 14, 8, 8, 8, 8)
CHUNKS = len(SHARES)
SUB = 640
ORDERS = ("xzy", "yzx", "xyz", "yxz", "xyz", "yxz")
SMALL = "xyz"
PIECES = 3


def factor(devices):
    chips = devices // 2
    log = chips.bit_length() - 1
    gx = 1 << (log // 3)
    gy = 1 << ((log - log // 3) // 2)
    return gx, gy, chips // (gx * gy)


def spans_of(coef):
    unit = sum(SHARES)
    pairs = -(-coef // (4 * LANES)) * 2
    ends = [sum(SHARES[:t + 1]) * pairs // unit for t in range(CHUNKS)]
    return [(end - start) * 2 * LANES for start, end in zip([0] + ends, ends)]


def column(row):
    rows = row.shape[1]
    line = lax.broadcasted_iota(jnp.int32, (rows, rows), 0)
    lane = lax.broadcasted_iota(jnp.int32, (rows, rows), 1)
    return jnp.sum(jnp.where(line == lane, row, 0.0), axis=1, keepdims=True)


def frequencies(first, width):
    index = (lax.broadcasted_iota(jnp.int32, (1, width), 1) + first).astype(jnp.float32)
    plane = jnp.floor((index + 0.5) * (1.0 / (GRID * GRID)))
    rest = index - plane * (GRID * GRID)
    col_x = jnp.floor((rest + 0.5) * (1.0 / GRID))
    col_z = rest - col_x * GRID
    freq_x = jnp.where(col_x >= GRID // 2, col_x - GRID, col_x)
    freq_z = jnp.where(col_z >= GRID // 2, col_z - GRID, col_z)
    return freq_x, plane, freq_z, index


def kernel(
    gx, gy, gz, spans, coef, total,
    part_hbm, ref_hbm, cls_hbm, orient_hbm, tilt_hbm,
    scores_ref, means_ref, load_ref,
    part, cls_ref, orient_ref, tilt_ref,
    low, all_ref, ready, small_send, small_recv, *rest,
):
    hop_sends, hop_recvs = rest[:3 * CHUNKS], rest[3 * CHUNKS:6 * CHUNKS]
    data, mine, send_core, recv_core = (rest[k * CHUNKS:(k + 1) * CHUNKS] for k in range(6, 10))
    extra = CHUNKS // 2
    core_pairs = recv_core[:CHUNKS // 2]
    recv_core = [core_pairs[t // 2].at[t % 2] for t in range(CHUNKS)]
    in_sems, ag_sems, core_sems, hop_sems, small_sems, send_sems = rest[10 * CHUNKS - extra:]
    starts = [sum(spans[:t]) for t in range(CHUNKS)]
    widths = [max(0, min(spans[t], coef - starts[t])) for t in range(CHUNKS)]
    me = lax.axis_index("dom")
    core = lax.rem(me, 2)
    chip = me // 2
    x = lax.rem(chip, gx)
    y = lax.rem(chip // gx, gy)
    z = chip // (gx * gy)
    sibling = me + 1 - 2 * core
    classes = 2 * gx * gy * gz
    half = classes // 2
    rows = part.shape[0]
    cut = coef // 2 // LANES * LANES

    def device(x_at, y_at, z_at, c_at):
        return ((z_at * gy + y_at) * gx + x_at) * 2 + c_at

    def x_peer(j):
        return device(lax.rem(x + j, gx), y, z, core)

    def y_peer(j):
        return device(x, lax.rem(y + j, gy), z, core)

    def x_cross(j):
        return device(lax.rem(x + j, gx), y, z, 1 - core)

    def y_cross(j):
        return device(x, lax.rem(y + j, gy), z, 1 - core)

    def z_cross(j):
        return device(x, y, lax.rem(z + j, gz), 1 - core)

    def z_peer(j):
        return device(x, y, lax.rem(z + j, gz), core)

    sizes = {"x": gx, "y": gy, "z": gz}
    peer_of = {"x": x_peer, "y": y_peer, "z": z_peer}
    cross_of = {"x": x_cross, "y": y_cross, "z": z_cross}

    def fetch(src, dst, at):
        copy = pltpu.make_async_copy(src, dst, in_sems.at[at])
        copy.start()
        return copy

    metas = [
        fetch(orient_hbm, orient_ref, 1),
        fetch(tilt_hbm, tilt_ref, 2),
        fetch(cls_hbm, cls_ref, 3),
    ]
    own_ref = fetch(ref_hbm.at[0], all_ref.at[0], 0)
    part_copies = []
    for t in range(0, CHUNKS, 2):
        cols = pl.ds(starts[t], widths[t] + widths[t + 1])
        part_copies.append(fetch(part_hbm.at[:, :, cols], part.at[:, :, cols], 4 + t // 2))

    barrier = pltpu.get_barrier_semaphore()
    peers = [sibling]
    peers += [x_peer(j) for j in range(1, gx)]
    peers += [y_peer(j) for j in range(1, gy)]
    peers += [z_peer(j) for j in range(1, gz)]
    peers += [x_cross(j) for j in range(1, gx)]
    peers += [y_cross(j) for j in range(1, gy)]
    peers += [z_cross(j) for j in range(1, gz)]
    for peer in peers:
        pl.semaphore_signal(barrier, inc=1, device_id=(peer,), device_id_type=MESH)

    def push(src, dst, send_sem, recv_sem, target):
        pltpu.make_async_remote_copy(
            src_ref=src, dst_ref=dst, send_sem=send_sem, recv_sem=recv_sem,
            device_id=(target,), device_id_type=MESH,
        ).start()

    def whole_of(ref, sem):
        return pltpu.make_async_remote_copy(
            src_ref=ref, dst_ref=ref, send_sem=sem, recv_sem=sem,
            device_id=(sibling,), device_id_type=MESH,
        )

    def arrived(ref, sem):
        whole_of(ref, sem).wait_recv()

    def slot(dx, dy, dc):
        return ((dc * gx + dx) * gy + dy) * gz

    def give(src_slot, dst_slot, n, lanes, at, target):
        src = all_ref.at[pl.ds(src_slot, n), :, lanes]
        dst = all_ref.at[pl.ds(dst_slot, n), :, lanes]
        push(src, dst, send_sems.at[0], ag_sems.at[at], target)

    every = slice(0, coef)
    front, back = slice(0, cut), slice(cut, coef)

    def split(g):
        return 1 + g * (gz - 1) // PIECES, 1 + (g + 1) * (gz - 1) // PIECES

    def sem_of(g):
        return 3 + 2 * (g + 1)

    cross = sem_of(PIECES)

    def ag_direct(g):
        at, end = split(g) if g >= 0 else (0, 1)
        sem = sem_of(g)
        if at == end:
            return
        for j in range(1, gx):
            give(at, slot(gx - j, 0, 1) + at, end - at, every, sem, x_cross(j))
        for j in range(1, gy):
            give(at, slot(0, gy - j, 1) + at, end - at, every, sem, y_cross(j))
        give(at, slot(0, 0, 1) + at, end - at, every, 0, sibling)

    def ag_forward(g):
        at, end = split(g) if g >= 0 else (0, 1)
        n, sem = end - at, sem_of(g)
        if n == 0:
            return
        if gx + gy > 2:
            arrived(all_ref.at[pl.ds(0, (gx + gy - 2) * n)], ag_sems.at[sem])
        for dx in range(1, gx):
            for j in range(1, gy):
                give(slot(dx, 0, 1) + at, slot(dx, gy - j, 1) + at, n, front, sem + 1, y_peer(j))
                if g == PIECES - 1:
                    give(slot(dx, 0, 1) + at, slot(dx, gy - j, 0) + at, n, front, cross, y_cross(j))
        for dy in range(1, gy):
            for j in range(1, gx):
                give(slot(0, dy, 1) + at, slot(gx - j, dy, 1) + at, n, back, sem + 1, x_peer(j))
                if g == PIECES - 1:
                    give(slot(0, dy, 1) + at, slot(gx - j, dy, 0) + at, n, back, cross, x_cross(j))
        for dx in range(1, gx):
            give(slot(dx, 0, 1) + at, slot(dx, 0, 0) + at, n, every, 0, sibling)
        for dy in range(1, gy):
            give(slot(0, dy, 1) + at, slot(0, dy, 0) + at, n, every, 0, sibling)

    def ag_core(g):
        at, end = split(g) if g >= 0 else (0, 1)
        n, sem = end - at, sem_of(g)
        count = (gx - 1) * (gy - 1) * n
        if count:
            arrived(all_ref.at[pl.ds(0, count)], ag_sems.at[sem + 1])
        if g == PIECES - 1:
            return
        for dx in range(1, gx):
            for dy in range(1, gy):
                give(slot(dx, dy, 1) + at, slot(dx, dy, 0) + at, n, every, 1, sibling)

    def ag_own():
        own_ref.wait()
        for j in range(1, gz):
            give(0, gz - j, 1, every, 2, z_peer(j))
        ag_direct(-1)

    def ag_z():
        if gz > 1:
            arrived(all_ref.at[pl.ds(1, gz - 1)], ag_sems.at[2])

    diag = (gx - 1) * (gy - 1) * gz
    early, late = [], []
    for dc in range(2):
        for dx in range(gx):
            for dy in range(gy):
                runs = late if dx and dy else early
                at = slot(dx, dy, dc)
                if runs and runs[-1][1] == at and at != half:
                    runs[-1] = (runs[-1][0], at + gz)
                else:
                    runs.append((at, at + gz))

    for copy in metas:
        copy.wait()
    angle = orient_ref[...].astype(jnp.float32) * (2.0 * math.pi / ORIENTS)
    bins = tilt_ref[...].astype(jnp.float32)
    low_end = -(40.0 + 1.5 * bins[0:1]) * (math.pi / 180.0)
    high_end = (40.0 + 1.5 * bins[1:2]) * (math.pi / 180.0)
    sin_a, cos_a = column(jnp.sin(angle)), column(jnp.cos(angle))
    cos_c = column(jnp.cos(low_end + high_end))
    sin_c = column(jnp.sin(low_end + high_end))
    cos_w = column(jnp.cos(high_end - low_end))
    cls_row = cls_ref[...].astype(jnp.float32)
    cls_col = column(cls_row)

    def log2(n):
        return n.bit_length() - 1

    row = lax.broadcasted_iota(jnp.int32, (classes, 1), 0)

    def ids_of(order, flip):
        left, at = row, {}
        for dim in reversed(order):
            at[dim] = left & (sizes[dim] - 1)
            left = lax.shift_right_logical(left, log2(sizes[dim]))
        return device((at["x"] + x) & (gx - 1), (at["y"] + y) & (gy - 1), (at["z"] + z) & (gz - 1), (left + core + flip) & 1)

    ids = ids_of("xyz", 0)
    onehot = {}
    for order in ORDERS:
        if order not in onehot:
            onehot[order] = jnp.where(ids_of(order, 1).astype(jnp.float32) == cls_row, 1.0, 0.0).astype(jnp.bfloat16)
    sums = {"wedge": jnp.zeros((rows, 1), jnp.float32), "power": jnp.zeros((rows, 1), jnp.float32)}

    def parts(first, size):
        width = max(0, min(size, coef - first))
        pieces = []
        if width:
            both = part[:, :, first:first + width].astype(jnp.float32)
            pieces.append(jnp.swapaxes(both, 0, 1))
        if width < size:
            pieces.append(jnp.zeros((2, rows, size - width), jnp.float32))
        both = jnp.concatenate(pieces, axis=2) if len(pieces) > 1 else pieces[0]
        return both[0], both[1]

    def wedges(first, size):
        freq_x, freq_y, freq_z, index = frequencies(first, size)
        along = freq_y * cos_a - freq_x * sin_a
        along_sq = along * along
        z_sq = freq_z * freq_z
        scale = 1.0 / (along_sq + (z_sq + 1.0))
        value = ((along_sq - z_sq) * cos_c - (2.0 * along * freq_z) * sin_c) * scale - cos_w
        wedge = 1.0 / (1.0 + jnp.exp(value * (-GAIN)))
        inside = wedge if first + size <= coef else jnp.where(index < coef, wedge, 0.0)
        sums["wedge"] = sums["wedge"] + jnp.sum(inside, axis=1, keepdims=True)
        return wedge

    def compute(t):
        span = spans[t]
        if t % 2 == 0:
            part_copies[t // 2].wait()
        for at in range(0, span, SUB):
            first = starts[t] + at
            size = min(SUB, span - at)
            wedge = wedges(first, size)
            real, imag = parts(first, size)
            sums["power"] = sums["power"] + jnp.sum(wedge * (real * real + imag * imag), axis=1, keepdims=True)
            data[t][:, at:at + size] = (wedge * real).astype(jnp.bfloat16)
            data[t][:, span + at:span + at + size] = (wedge * imag).astype(jnp.bfloat16)
            data[t][:, 2 * span + at:2 * span + at + size] = (wedge * wedge).astype(jnp.bfloat16)
            low[:, first:first + size] = wedge.astype(jnp.bfloat16)
        for q in range(3):
            cols = slice(q * span, (q + 1) * span)
            both = jnp.dot(onehot[ORDERS[t]], data[t][:, cols], preferred_element_type=jnp.float32)
            send_core[t][:, cols] = both[half:].astype(jnp.bfloat16)
            mine[t][:, cols] = both[:half]

    def cores(t):
        push(send_core[t], recv_core[t], send_sems.at[1], core_sems.at[t // 2], sibling)

    def fold(line):
        wide = line.shape[1]
        return jnp.concatenate([line[:, :wide // 2], line[:, wide // 2:]], axis=0)

    def taken(t, k):
        if k < 0:
            if t % 2 == 0:
                arrived(core_pairs[t // 2], core_sems.at[t // 2])
            return mine[t][...] + recv_core[t][...].astype(jnp.float32)
        n = sizes[ORDERS[t][k]]
        lines = math.prod(sizes[dim] for dim in ORDERS[t][k + 1:])
        recv = hop_recvs[3 * t + k]
        if k == 1 or n > 1:
            arrived(recv, hop_sems.at[3 * t + k])
        if k == 1:
            piece = recv[0].astype(jnp.float32)
            for j in range(1, n):
                piece = piece + recv[j].astype(jnp.float32)
            return piece
        piece = mine[t][:lines]
        if lines == 1:
            piece = fold(piece)
        for j in range(1, n):
            piece = piece + recv[j - 1].astype(jnp.float32)
        return piece

    def hop(t, k):
        dim = ORDERS[t][k]
        lines = math.prod(sizes[dim] for dim in ORDERS[t][k + 1:])
        piece = taken(t, k - 1)
        send, recv = hop_sends[3 * t + k], hop_recvs[3 * t + k]
        for j in range(0 if k == 1 else 1, sizes[dim]):
            part_of = piece[j * lines:(j + 1) * lines]
            if lines == 1:
                part_of = fold(part_of)
            at = j if k == 1 else j - 1
            send[at] = part_of.astype(jnp.bfloat16)
            peer = sibling if j == 0 else (cross_of if k == 1 else peer_of)[dim](j)
            sem = 4 if j == 0 else 2
            push(send.at[at], recv.at[at], send_sems.at[sem], hop_sems.at[3 * t + k], peer)
        if k != 1:
            mine[t][:lines] = piece[:lines]

    def first(t):
        hop(t, 0)

    def second(t):
        hop(t, 1)

    def third(t):
        hop(t, 2)

    reach = small_send.shape[2] // 2
    stages = [(1, lambda j: sibling)] + [(sizes[dim] - 1, (peer_of, cross_of, peer_of)[k][dim]) for k, dim in enumerate(SMALL)]

    def small_start():
        lane = lax.broadcasted_iota(jnp.int32, (rows, reach), 1).astype(jnp.float32)
        hits = jnp.where(lane == cls_col, 1.0, 0.0)
        small_send[0, :, :reach] = jnp.sum(hits, axis=0, keepdims=True)
        small_send[0, :, reach:] = jnp.sum(hits * sums["wedge"], axis=0, keepdims=True)
        small_push(0)

    def small_push(k):
        at = sum(n for n, _ in stages[:k])
        for j in range(stages[k][0]):
            push(small_send.at[k], small_recv.at[at + j], send_sems.at[3], small_sems.at[k], stages[k][1](j + 1))

    def small_take(k):
        at, n = sum(n for n, _ in stages[:k]), stages[k][0]
        tally = small_send[k]
        if n:
            arrived(small_recv.at[pl.ds(at, n)], small_sems.at[k])
        for j in range(n):
            tally = tally + small_recv[at + j]
        return tally

    def small_next(k):
        small_send[k + 1] = small_take(k)
        small_push(k + 1)

    nt = (((1,), (1,)), ((), ()))
    table = []

    def position(at):
        before = 0
        for begin, end in early + late:
            if begin <= at < end:
                return before + at - begin
            before += end - begin

    order = jnp.concatenate([ids[begin:end] for begin, end in early + late], axis=0)

    def prepare(runs):
        for begin, end in runs:
            lines = slice(begin, end)
            for t in range(CHUNKS):
                cols = slice(starts[t], starts[t] + widths[t])
                both = jnp.swapaxes(all_ref[lines, :, cols].astype(jnp.float32), 0, 1)
                real, imag = both[0], both[1]
                to = slice(position(begin), position(begin) + end - begin)
                ready[0, to, cols] = real.astype(jnp.bfloat16)
                ready[1, to, cols] = imag.astype(jnp.bfloat16)
                ready[2, to, cols] = (real * real + imag * imag).astype(jnp.bfloat16)

    def score(begin, end):
        power = sums["power"]
        for at in range(begin, end, 32):
            lines = slice(at, min(at + 32, end))
            group = lines.stop - lines.start
            inter = jnp.zeros((rows, group), jnp.float32)
            energy = jnp.zeros((rows, group), jnp.float32)
            for t in range(CHUNKS):
                width, span = widths[t], spans[t]
                cols = slice(starts[t], starts[t] + width)
                inter = inter + lax.dot_general(data[t][:, :width], ready[0, lines, cols], nt, preferred_element_type=jnp.float32)
                inter = inter + lax.dot_general(data[t][:, span:span + width], ready[1, lines, cols], nt, preferred_element_type=jnp.float32)
                energy = energy + lax.dot_general(low[:, cols], ready[2, lines, cols], nt, preferred_element_type=jnp.float32)
            value = inter / (math.sqrt(coef) * jnp.sqrt((energy / coef + EPS) * (power / coef + EPS)))
            lane = lax.broadcasted_iota(jnp.int32, (group, classes), 1)
            place = jnp.where(order[lines] == lane, 1.0, 0.0)
            table.append(jnp.dot(value, place, precision=lax.Precision.HIGHEST, preferred_element_type=jnp.float32))

    groups = [(at, at + gz) for begin, end in early for at in range(begin, end, gz)]

    def merged(runs):
        out = []
        for begin, end in runs:
            if out and out[-1][1] == begin and begin != half:
                out[-1] = (out[-1][0], end)
            else:
                out.append((begin, end))
        return out

    def prepare_near():
        prepare(merged([g for g in groups if (g[0] < half) == (g[0] % half == 0)]))

    def prepare_far():
        arrived(all_ref.at[pl.ds(0, half - diag)], ag_sems.at[0])
        prepare(merged([g for g in groups if (g[0] < half) != (g[0] % half == 0)]))

    def score_late():
        last = (gx - 1) * (gy - 1) * (gz - split(PIECES - 1)[0])
        if diag > last:
            arrived(all_ref.at[pl.ds(0, diag - last)], ag_sems.at[1])
        if last:
            arrived(all_ref.at[pl.ds(0, last)], ag_sems.at[cross])
        prepare(late)
        score(classes - 2 * diag, classes)
        scores_ref[...] = sum(table[1:], table[0])

    floors = []

    def counts():
        tally = small_take(3)
        load_ref[...] = tally[:, :classes] * classes / total
        lane = lax.broadcasted_iota(jnp.int32, (1, reach), 1)
        wedge_total = jnp.sum(jnp.where(lane == me, tally[:, reach:], 0.0), axis=1, keepdims=True)
        floors.append(TAU * (wedge_total / coef + 1.0))

    def means(t):
        whole = taken(t, 2)
        flat = jnp.concatenate([whole[0:1], whole[1:2]], axis=1)
        span, width, start = spans[t], widths[t], starts[t]
        scale = 1.0 / (flat[:, 2 * span:2 * span + width] + floors[0])
        for q in range(2):
            means_ref[0, q:q + 1, start:start + width] = flat[:, q * span:q * span + width] * scale

    compute(0)
    pl.semaphore_wait(barrier, len(peers))
    ag_own()
    cores(0)
    compute(1)
    cores(1)
    compute(2)
    cores(2)
    compute(3)
    cores(3)
    hop(0, 0)
    hop(1, 0)
    compute(4)
    cores(4)
    compute(5)
    cores(5)
    small_start()
    hop(2, 0)
    hop(3, 0)
    small_next(0)
    hop(4, 0)
    hop(5, 0)
    ag_forward(-1)
    hop(0, 1)
    hop(1, 1)
    ag_z()
    ag_direct(0)
    ag_direct(1)
    ag_direct(2)
    hop(2, 1)
    hop(3, 1)
    small_next(1)
    hop(4, 1)
    hop(5, 1)
    ag_forward(0)
    ag_forward(1)
    ag_forward(2)
    hop(2, 2)
    hop(3, 2)
    small_next(2)
    hop(4, 2)
    hop(5, 2)
    ag_core(-1)
    hop(0, 2)
    hop(1, 2)
    prepare_near()
    ag_core(0)
    prepare_far()
    score(0, classes - 2 * diag)
    ag_core(1)
    ag_core(2)
    score_late()
    counts()
    means(0)
    means(1)
    means(2)
    means(3)
    means(4)
    means(5)

    whole_of(all_ref.at[pl.ds(0, classes - 1)], send_sems.at[0]).wait_send()
    whole_of(ready.at[:, :half, :], send_sems.at[1]).wait_send()
    whole_of(all_ref.at[pl.ds(0, classes - 2), :, :3 * sum(spans) // 4], send_sems.at[2]).wait_send()
    whole_of(small_recv, send_sems.at[3]).wait_send()
    kept = sum(3 * spans[t] * sizes[ORDERS[t][2]] for t in range(CHUNKS)) // (2 * LANES)
    lines = next(n for n in range(classes, 0, -1) if kept % n == 0 and kept // n * LANES <= coef)
    whole_of(all_ref.at[pl.ds(0, lines), :, :kept // lines * LANES], send_sems.at[4]).wait_send()


def finish(*arrays):
    n = len(arrays)

    def put(*refs):
        sems = refs[2 * n]
        copies = [pltpu.make_async_copy(refs[i], refs[n + i], sems.at[i]) for i in range(n)]
        for copy in copies:
            copy.start()
        for copy in copies:
            copy.wait()

    scores, means, load = pl.pallas_call(
        put,
        out_shape=tuple(jax.ShapeDtypeStruct(a.shape, a.dtype) for a in arrays),
        in_specs=[pl.BlockSpec(memory_space=pltpu.VMEM)] * n,
        out_specs=(pl.BlockSpec(memory_space=pltpu.HBM),) * n,
        scratch_shapes=[pltpu.SemaphoreType.DMA((n,))],
        compiler_params=pltpu.CompilerParams(vmem_limit_bytes=1024 * 1024),
    )(*arrays)
    return (scores, means, load[0])


def body(particles, references, assignment, orientation, tilt_range):
    part_rows = particles.shape[0]
    coef = particles.shape[2]
    devices = lax.axis_size("dom")
    classes = references.shape[0] * devices
    assert references.shape[0] == 1
    gx, gy, gz = factor(devices)
    total = part_rows * devices
    spans = spans_of(coef)
    padded = sum(spans)
    width = 2 * (-(-classes // LANES) * LANES)
    half = classes // 2

    vmem = pl.BlockSpec(memory_space=pltpu.VMEM)
    hbm = pl.BlockSpec(memory_space=pltpu.HBM)
    dma = pltpu.SemaphoreType.DMA
    bf16, f32, i32 = jnp.bfloat16, jnp.float32, jnp.int32

    sizes = {"x": gx, "y": gy, "z": gz}
    hops = []
    for order, span in zip(ORDERS, spans):
        wide = 3 * span
        for k, dim in enumerate(order):
            lines = math.prod(sizes[d] for d in order[k + 1:])
            shape = (lines, wide) if lines > 1 else (2, wide // 2)
            hops.append(((max(1, sizes[dim] - (k != 1)), *shape), bf16))
    buffers = [
        ((part_rows, 2, coef), bf16),
        ((1, part_rows), i32),
        ((1, part_rows), i32),
        ((2, part_rows), i32),
        ((part_rows, padded), bf16),
        ((classes, 2, coef), bf16),
        ((3, classes, padded), bf16),
        ((4, 1, width), f32),
        ((gx + gy + gz - 2, 1, width), f32),
        *hops, *hops,
        *[((part_rows, 3 * span), bf16) for span in spans],
        *[((half, 3 * span), f32) for span in spans],
        *[((half, 3 * span), bf16) for span in spans],
        *[((2, half, 3 * span), bf16) for span in spans[::2]],
    ]
    held = sum(math.prod(shape) * jnp.dtype(kind).itemsize for shape, kind in buffers)
    limit = min(60, held // 2**20 + 8) * 2**20
    scores, means, load = pl.pallas_call(
        functools.partial(kernel, gx, gy, gz, spans, coef, total),
        out_shape=(
            jax.ShapeDtypeStruct((part_rows, classes), f32),
            jax.ShapeDtypeStruct((1, 2, coef), f32),
            jax.ShapeDtypeStruct((1, classes), f32),
        ),
        in_specs=[hbm] * 5,
        out_specs=(vmem, vmem, vmem),
        scratch_shapes=[pltpu.VMEM(shape, kind) for shape, kind in buffers] + [
            dma((4 + CHUNKS // 2,)), dma((3 + 2 * (PIECES + 1) + 1,)), dma((CHUNKS // 2,)), dma((3 * CHUNKS,)), dma((4,)), dma((5,)),
        ],
        compiler_params=pltpu.CompilerParams(
            collective_id=0, has_side_effects=True, vmem_limit_bytes=limit
        ),
    )(*[
        pltpu.with_memory_space_constraint(v, pltpu.HBM)
        for v in (particles, references, assignment.reshape(1, part_rows), orientation[None, :], tilt_range)
    ])
    return finish(scores, means, load)


def solution(mesh):
    in_specs = (
        P("dom", None, None),
        P("dom", None, None),
        P("dom", None),
        P("dom"),
        P(None, "dom"),
    )
    out_specs = (P("dom", None), P("dom", None, None), P())
    return jax.shard_map(body, mesh=mesh, in_specs=in_specs, out_specs=out_specs, check_vma=False)
```
